256 devices in a mesh: dom: 128 (over x, z, y), mp: 2 (over core).
Axes of the slice: x: 4, y: 4, z: 8, core: 2. Of those that a mesh axis runs over, the one named last changes fastest.
Arguments:
- table: bfloat16 [524288, 768], P('dom', 'mp'), may hold values from -6 to 6
- weight_a: bfloat16 [1536, 512], P(None, 'mp'), may hold values from -0.15625 to 0.15625
- bias_a: float32 [512], replicated, may hold values from -3 to 3
- weight_b: bfloat16 [1024, 512], P(None, 'mp'), may hold values from -0.25 to 0.25
- bias_b: float32 [512], replicated, may hold values from -3 to 3
- requests: int32 [128, 128, 16], P('dom'), may hold values from 0 to 4095
- near_a: int32 [131072, 10], P('dom'), may hold values from 0 to 2047
- self_a: int32 [131072], P('dom'), may hold values from 0 to 2047
- count_a: int32 [131072], P('dom'), may hold values from 1 to 10
- near_b: int32 [32768, 5], P('dom'), may hold values from 0 to 1023
- self_b: int32 [32768], P('dom'), may hold values from 0 to 1023
- count_b: int32 [32768], P('dom'), may hold values from 1 to 5
Outputs:
- embedding: bfloat16 [32768, 512], P('dom', 'mp')
The draws below stay inside these ranges and needn't reach their ends.
Inputs may be any that keep to these rules, and one draw needn't show every extreme that they name: `requests`: local row indices at the owner. `near_a`: slots of the same minibatch; entries at j >= count_a are padding. `near_b`: positions within the same minibatch; entries at j >= count_b are padding.
All inputs are finite; a program needn't handle non-finite values.
Results may differ from the reference program's by a relative error of at most 0.0074.
Values may be sent and summed in bfloat16 or wider, within the bound.
A program may use at most 64 MiB of HBM per device.

```python
import jax
import jax.numpy as jnp
from jax import lax

F = 768
H = 512
FAN_A = 10
FAN_B = 5
SEEDS_DEV = 256
NODE_DEV = 4096
HOP_DEV = 1024
SLOTS_DEV = 2048
NODES = 524288
HOPS = 131072
SEEDS = 32768
N_DOM = 128


def set_ends(values, stream_key, smallest, high):
    index_at = [jax.random.randint(jax.random.fold_in(stream_key, axis), (), 0, length) for axis, length in enumerate(values.shape)]
    widest = values.shape.index(max(values.shape))
    beside = index_at[:widest] + [(index_at[widest] + 1) % values.shape[widest]] + index_at[widest + 1:]
    return values.at[tuple(index_at)].set(smallest).at[tuple(beside)].set(high)


def level_of(rng, dims, split, smallest, high):
    def one(axis_at, blocks):
        heights = jax.random.uniform(jax.random.fold_in(jax.random.fold_in(rng, 6), axis_at), (blocks,), jnp.float32, smallest / len(split), high / len(split))
        return jnp.repeat(jnp.exp(heights), dims[axis_at] // blocks).reshape((-1,) + (1,) * (len(dims) - axis_at - 1))

    level = one(*split[0])
    for cut in split[1:]:
        level = level * one(*cut)
    return level


def centred(rng, dims, width, most, shards=(), kind=jnp.bfloat16):
    loudness = level_of(rng, dims, shards, -0.22, 0.18) if shards else 1.0
    values = jax.random.normal(rng, dims, jnp.float32) * width * loudness
    return jnp.minimum(jnp.maximum(values, -most), most).astype(kind)


def setup_inputs(seed: int = 0) -> dict:
    splits = jax.random.split(jax.random.key(seed), 13)
    table = centred(splits[0], (NODES, F), 1.0, 6.0, ((0, 128), (1, 2)))
    weight_a = centred(splits[1], (2 * F, H), (2 * F) ** -0.5, 0.15625, ((1, 2),))
    bias_a = centred(splits[2], (H,), 0.5, 3.0, (), jnp.float32)
    weight_b = centred(splits[3], (2 * H, H), H ** -0.5, 0.25, ((1, 2),))
    bias_b = centred(splits[4], (H,), 0.5, 3.0, (), jnp.float32)
    requests = set_ends(jax.random.randint(splits[5], (N_DOM, N_DOM, SLOTS_DEV // N_DOM), 0, NODE_DEV), jax.random.fold_in(splits[5], 1), 0, NODE_DEV - 1).astype(jnp.int32)
    near_a = set_ends(jax.random.randint(splits[6], (HOPS, FAN_A), 0, SLOTS_DEV), jax.random.fold_in(splits[6], 1), 0, SLOTS_DEV - 1).astype(jnp.int32)
    self_a = set_ends(jax.random.randint(splits[7], (HOPS,), 0, SLOTS_DEV), jax.random.fold_in(splits[7], 1), 0, SLOTS_DEV - 1).astype(jnp.int32)
    count_a = set_ends(jax.random.randint(splits[8], (HOPS,), 1, FAN_A + 1), jax.random.fold_in(splits[8], 1), 1, FAN_A).astype(jnp.int32)
    near_b = set_ends(jax.random.randint(splits[9], (SEEDS, FAN_B), 0, HOP_DEV), jax.random.fold_in(splits[9], 1), 0, HOP_DEV - 1).astype(jnp.int32)
    self_b = set_ends(jax.random.randint(splits[10], (SEEDS,), 0, HOP_DEV), jax.random.fold_in(splits[10], 1), 0, HOP_DEV - 1).astype(jnp.int32)
    count_b = set_ends(jax.random.randint(splits[11], (SEEDS,), 1, FAN_B + 1), jax.random.fold_in(splits[11], 1), 1, FAN_B).astype(jnp.int32)
    return {"table": table, "weight_a": weight_a, "bias_a": bias_a, "weight_b": weight_b, "bias_b": bias_b, "requests": requests, "near_a": near_a, "self_a": self_a, "count_a": count_a, "near_b": near_b, "self_b": self_b, "count_b": count_b}


def mean_rows(source, neighbours, counts):
    running = jnp.zeros((neighbours.shape[0], source.shape[1]), jnp.float32)
    for column in range(neighbours.shape[1]):
        keep_mask = (counts > column)[:, None]
        running = running + jnp.where(keep_mask, source[neighbours[:, column]].astype(jnp.float32), 0.0)
    return (running / counts[:, None].astype(jnp.float32)).astype(jnp.bfloat16)

def reference(table, weight_a, bias_a, weight_b, bias_b, requests, near_a, self_a, count_a, near_b, self_b, count_b):
    offsets = (jnp.arange(N_DOM) * NODE_DEV).astype(jnp.int32)[:, None]

    def per_device(blocks):
        asked, hop_near, hop_self, hop_count, seed_near, seed_self, seed_count = blocks
        row_ids = (asked + offsets).reshape(-1).astype(jnp.int32)
        fetched = table[row_ids]
        mean_a = mean_rows(fetched, hop_near, hop_count)
        inputs_a = jnp.concatenate([fetched[hop_self], mean_a], axis=1)
        before = jnp.dot(inputs_a, weight_a, preferred_element_type=jnp.float32) + bias_a
        hidden_a = jax.nn.relu(before).astype(jnp.bfloat16)
        mean_b = mean_rows(hidden_a, seed_near, seed_count)
        inputs_b = jnp.concatenate([hidden_a[seed_self], mean_b], axis=1)
        state = jax.nn.relu(jnp.dot(inputs_b, weight_b, preferred_element_type=jnp.float32) + bias_b)
        squares = lax.optimization_barrier(jnp.sum(state * state, axis=1, keepdims=True))
        return (state * jnp.sqrt(jnp.float32(H)) / jnp.sqrt(squares + H)).astype(jnp.bfloat16)
    blocks = (requests, near_a.reshape(N_DOM, HOP_DEV, FAN_A), self_a.reshape(N_DOM, HOP_DEV), count_a.reshape(N_DOM, HOP_DEV), near_b.reshape(N_DOM, SEEDS_DEV, FAN_B), self_b.reshape(N_DOM, SEEDS_DEV), count_b.reshape(N_DOM, SEEDS_DEV))
    result = lax.map(per_device, blocks)
    return result.reshape(N_DOM * SEEDS_DEV, H)
```

```python
import functools

import jax
import jax.numpy as jnp
from jax import lax
from jax.experimental import pallas as pl
from jax.experimental.pallas import tpu as pltpu
from jax.sharding import PartitionSpec as P

F = 768
H = 512
FH = 384
HH = 256
NX, NY, NZ = 4, 4, 8
NP = NX * NY
ROWS = 16
HOP = 1024
SLOTS = 2048
SEEDS = 256
NODE = 4096
BLK = 256
NBLK = HOP // BLK
MESH = pl.DeviceIdType.MESH
I32 = jnp.int32
F32 = jnp.float32
BF = jnp.bfloat16


def kernel(
    table, wa, ba, wb, bb, req, near_a, self_a, cnt_a, near_b, self_b, cnt_b,
    out,
    table_v, wa_v, wb_v, req_v, near_v, selfa_v, cnta_v, nearb_v, selfb_v, cntb_v,
    req2, zreq, tz, pick, stag, xbuf, amat, acc, lo_s, w0_s, w1_s, selfc, invc,
    part, psend, precv, bmat, accb, invb,
    lsem, wsem, wrsem, psem, prsem, zsem, zrsem, fsem, frsem, qsem, qrsem,
):
    d = lax.axis_index("dom")
    c = lax.axis_index("mp")
    x, z, y = d // (NZ * NY), (d // NY) % NZ, d % NY
    qme = x * NY + y
    mate = (d, 1 - c)

    def at_plane(m):
        tx = (x + m // NY) % NX
        ty = (y + m % NY) % NY
        return tx, ty, tx * NY + ty

    def dev(tx, tz_, ty):
        return (tx * (NZ * NY) + tz_ * NY + ty, c)

    local = []

    def bring(src, dst):
        cp = pltpu.make_async_copy(src, dst, lsem.at[len(local)])
        cp.start()
        local.append(cp)
        return cp

    c_req = bring(req, req_v)
    c_idx = [bring(near_a, near_v), bring(self_a, selfa_v), bring(cnt_a, cnta_v)]
    c_tab = bring(table, table_v)
    c_idb = [bring(near_b, nearb_v), bring(self_b, selfb_v), bring(cnt_b, cntb_v)]
    mine = pl.multiple_of(c * FH, 128)
    c_w = [
        bring(wa.at[pl.ds(mine, FH)], wa_v.at[c, pl.ds(0, FH)]),
        bring(wa.at[pl.ds(F + mine, FH)], wa_v.at[c, pl.ds(FH, FH)]),
        bring(wb, wb_v.at[c]),
    ]

    barrier = pltpu.get_barrier_semaphore()
    for m in range(1, NP):
        tx, ty, _ = at_plane(m)
        pl.semaphore_signal(barrier, inc=1, device_id=dev(tx, z, ty), device_id_type=MESH)
    for j in range(1, NZ):
        pl.semaphore_signal(barrier, inc=1, device_id=dev(x, (z + j) % NZ, y), device_id_type=MESH)
    pl.semaphore_signal(barrier, inc=1, device_id=mate, device_id_type=MESH)

    c_req.wait()
    r = req_v[...]
    rows2 = jnp.concatenate(
        [
            jnp.concatenate([r[a * 32 + k * 4 : a * 32 + k * 4 + 4, :] for a in range(NX)], axis=0)
            for k in range(NZ)
        ],
        axis=1,
    )
    req2[...] = rows2.reshape(NP, 1, 128)

    for cp in c_idx:
        cp.wait()

    def place(s):
        kk = (((s >> 6) & 7) - z) & 7
        return (kk << 8) | ((s >> 9) << 6) | (s & 63)

    self_t = place(selfa_v[...]).T
    cnt_t = cnta_v[...].T
    for g in range(HOP // 128):
        rows = pl.ds(g * 128, 128)
        cnt = cnt_t[:, g : g + 1]
        selfc[rows, :] = self_t[:, g : g + 1]
        invc[rows, :] = 1.0 / cnt.astype(F32)
        p = place(near_v[rows, :])
        valid = lax.broadcasted_iota(I32, p.shape, 1) < cnt
        one = jnp.left_shift(jnp.ones_like(p), ((p >> 7) & 7) * 4)
        lo_s[rows, :] = p & 127
        w0_s[rows, :] = jnp.where(valid & (p < 1024), one, 0)
        w1_s[rows, :] = jnp.where(valid & (p >= 1024), one, 0)

    pl.semaphore_wait(barrier, NP - 1 + NZ - 1 + 1)

    for m in range(1, NP):
        tx, ty, q = at_plane(m)
        pltpu.make_async_remote_copy(
            src_ref=req2.at[q], dst_ref=zreq.at[0, qme], send_sem=psem, recv_sem=prsem,
            device_id=dev(tx, z, ty), device_id_type=MESH,
        ).start()
    zreq[0, qme] = req2[qme]

    lanes = lax.broadcasted_iota(I32, (16, 128), 1)

    def build(rb, _):
        rows = pl.ds(pl.multiple_of(rb * 16, 16), 16)
        rows_s = pl.ds(pl.multiple_of(HOP + rb * 16, 16), 16)
        lo, w0, w1 = lo_s[rows, :], w0_s[rows, :], w1_s[rows, :]
        a0 = jnp.zeros((16, 128), I32)
        a1 = jnp.zeros((16, 128), I32)
        for j in range(lo.shape[1]):
            hit = lo[:, j : j + 1] == lanes
            a0 = a0 + jnp.where(hit, w0[:, j : j + 1], 0)
            a1 = a1 + jnp.where(hit, w1[:, j : j + 1], 0)
        own = jnp.broadcast_to(selfc[rows, :], (16, 128))
        for t in range(SLOTS // 128):
            word = a0 if t < 8 else a1
            v = jnp.right_shift(word, 4 * (t % 8)) & 15
            cols = pl.ds(t * 128, 128)
            amat[rows, cols] = v.astype(F32).astype(BF)
            amat[rows_s, cols] = jnp.where(own == lanes + t * 128, 1.0, 0.0).astype(BF)
        return 0

    lax.fori_loop(0, HOP // 16, build, 0)

    got = pltpu.make_async_remote_copy(
        src_ref=req2.at[pl.ds(0, NP - 1)], dst_ref=zreq.at[0, pl.ds(0, NP - 1)],
        send_sem=psem, recv_sem=prsem, device_id=mate, device_id_type=MESH,
    )
    got.wait_recv()

    def z_copy(j):
        return pltpu.make_async_remote_copy(
            src_ref=zreq.at[0], dst_ref=zreq.at[(NZ - j) % NZ],
            send_sem=zsem.at[j], recv_sem=zrsem.at[(NZ - j) % NZ],
            device_id=dev(x, (z + j) % NZ, y), device_id_type=MESH,
        )

    for j in (1, 7, 2, 6, 3, 5, 4):
        z_copy(j).start()

    other = pl.multiple_of((1 - c) * FH, 128)
    w_out = []
    for i, (src, dst) in enumerate(
        (
            (wa.at[pl.ds(other, FH)], wa_v.at[c, pl.ds(0, FH)]),
            (wa.at[pl.ds(F + other, FH)], wa_v.at[c, pl.ds(FH, FH)]),
            (wb, wb_v.at[c]),
        )
    ):
        cp = pltpu.make_async_remote_copy(
            src_ref=src, dst_ref=dst, send_sem=wsem.at[i], recv_sem=wrsem.at[i],
            device_id=mate, device_id_type=MESH,
        )
        cp.start()
        w_out.append(cp)

    c_tab.wait()

    def order(i):
        return (i % 2) * ((i + 1) // 2) + (1 - i % 2) * ((NZ - i // 2) % NZ)

    def feature_send(k, m):
        tx, ty, q = at_plane(m)
        kk = (NZ - k) % NZ
        return pltpu.make_async_remote_copy(
            src_ref=stag.at[k * NP + q], dst_ref=xbuf.at[kk * NP + qme],
            send_sem=fsem.at[k], recv_sem=frsem.at[kk],
            device_id=dev(tx, (z + k) % NZ, ty), device_id_type=MESH,
        )

    def gather(k):
        tz[...] = zreq[k].reshape(NP, 128).T
        idx = tz[pl.ds(pl.multiple_of(z * 16, 16), 16), :]
        for q in range(NP):
            want = jnp.broadcast_to(idx[:, q : q + 1], (16, 128))
            for t in range(NODE // 128):
                pick[pl.ds(q * 16, 16), pl.ds(t * 128, 128)] = jnp.where(
                    want == lanes + t * 128, 1.0, 0.0
                ).astype(BF)
        rows = jnp.dot(pick[...], table_v[...], preferred_element_type=F32)
        stag[pl.ds(k * NP, NP)] = rows.astype(BF).reshape(NP, ROWS, FH)

    def serve(i, _):
        k = order(i)

        @pl.when(i > 0)
        def _():
            pltpu.make_async_remote_copy(
                src_ref=zreq.at[0], dst_ref=zreq.at[k], send_sem=zsem.at[0], recv_sem=zrsem.at[k],
                device_id=mate, device_id_type=MESH,
            ).wait_recv()

        gather(k)

        @pl.when(i > 0)
        def _():
            feature_send(k, 0).start()

        for m in range(1, NP):
            feature_send(k, m).start()
        return 0

    lax.fori_loop(0, NZ, serve, 0)
    xbuf[qme] = stag[qme]

    for cp in c_idb:
        cp.wait()
    selfb_t = selfb_v[...].T
    cntb_t = cntb_v[...].T
    for g in range(SEEDS // 128):
        cnt = cntb_t[:, g : g + 1]
        invb[pl.ds(g * 128, 128), :] = 1.0 / cnt.astype(F32)
        nb = nearb_v[pl.ds(g * 128, 128), :]
        nb = jnp.where(lax.broadcasted_iota(I32, nb.shape, 1) < cnt, nb, -1)
        sb = selfb_t[:, g : g + 1]
        for s in range(8):
            for t in range(HOP // 128):
                tot = jnp.zeros((16, 128), F32)
                for j in range(nb.shape[1]):
                    tot = tot + jnp.where(nb[s * 16 : s * 16 + 16, j : j + 1] == lanes + t * 128, 1.0, 0.0)
                bmat[pl.ds(g * 128 + s * 16, 16), pl.ds(t * 128, 128)] = tot.astype(BF)
                hit = sb[s * 16 : s * 16 + 16] == lanes + t * 128
                bmat[pl.ds(SEEDS + g * 128 + s * 16, 16), pl.ds(t * 128, 128)] = jnp.where(
                    hit, 1.0, 0.0
                ).astype(BF)

    def add_up(k, first):
        xk = xbuf[pl.ds(k * NP, NP)].reshape(BLK, FH)

        def rows_of(b, _):
            rows = pl.ds(pl.multiple_of(b * 512, 512), 512)
            cols = pl.ds(pl.multiple_of(k * BLK, BLK), BLK)
            tot = jnp.dot(amat[rows, cols], xk, preferred_element_type=F32)
            if first:
                acc[rows, :] = tot
            else:
                acc[rows, :] += tot
            return 0

        lax.fori_loop(0, SLOTS // 512, rows_of, 0)

    def arrived(k, n):
        pltpu.make_async_remote_copy(
            src_ref=stag.at[pl.ds(0, n)], dst_ref=xbuf.at[pl.ds(k * NP, n)],
            send_sem=fsem.at[0], recv_sem=frsem.at[k], device_id=mate, device_id_type=MESH,
        ).wait_recv()

    arrived(0, NP - 1)
    add_up(0, True)

    def collect(i, _):
        k = order(i)
        arrived(k, NP)
        add_up(k, False)
        return 0

    lax.fori_loop(1, NZ, collect, 0)

    for cp in c_w:
        cp.wait()
    for cp in w_out:
        cp.wait_recv()

    def half_copy(b):
        return pltpu.make_async_remote_copy(
            src_ref=psend.at[b], dst_ref=precv.at[b], send_sem=qsem.at[b], recv_sem=qrsem.at[b],
            device_id=mate, device_id_type=MESH,
        )

    for b in range(NBLK):
        rows = pl.ds(b * BLK, BLK)
        own = acc[pl.ds(HOP + b * BLK, BLK), :].astype(BF)
        mean = (acc[rows, :] * invc[rows, :]).astype(BF)
        both = jnp.concatenate([own, mean], axis=1)
        for h in range(2):
            v = jnp.dot(both, wa_v[h], preferred_element_type=F32)
            part[rows, pl.ds(h * HH, HH)] = v
            psend[b, :, pl.ds(h * HH, HH)] = v.astype(BF)
        half_copy(b).start()

    for b in range(NBLK):
        rows = pl.ds(b * BLK, BLK)
        half_copy(b).wait_recv()
        v = part[rows, :] + precv[b].astype(F32) + ba[...]
        hid = jnp.maximum(v, 0.0).astype(BF)
        tot = jnp.dot(bmat[:, pl.ds(b * BLK, BLK)], hid, preferred_element_type=F32)
        if b == 0:
            accb[...] = tot
        else:
            accb[...] += tot

    own = accb[pl.ds(SEEDS, SEEDS), :].astype(BF)
    mean = (accb[pl.ds(0, SEEDS), :] * invb[...]).astype(BF)
    both = jnp.concatenate([own, mean], axis=1)

    def state_of(h):
        v = jnp.dot(both, wb_v[h], preferred_element_type=F32) + bb[pl.ds(h, 1), :]
        return jnp.maximum(v, 0.0)

    s0 = state_of(c)
    s1 = state_of(1 - c)
    squares = jnp.sum(s0 * s0, axis=1, keepdims=True) + jnp.sum(s1 * s1, axis=1, keepdims=True)
    out[...] = (s0 * jnp.sqrt(jnp.float32(H)) / jnp.sqrt(squares + H)).astype(BF)

    got.wait_send()
    for j in range(1, NZ):
        z_copy(j).wait_send()
    for cp in w_out:
        cp.wait_send()
    for k in range(NZ):
        n = NP - 1 if k == 0 else NP
        pltpu.make_async_remote_copy(
            src_ref=stag.at[pl.ds(k * NP, n)], dst_ref=xbuf.at[pl.ds(0, n)],
            send_sem=fsem.at[k], recv_sem=frsem.at[0], device_id=mate, device_id_type=MESH,
        ).wait_send()
    for b in range(NBLK):
        half_copy(b).wait_send()


def shards(
    table, weight_a, bias_a, weight_b, bias_b, requests,
    near_a, self_a, count_a, near_b, self_b, count_b,
):
    vmem = pl.BlockSpec(memory_space=pltpu.VMEM)
    hbm = pl.BlockSpec(memory_space=pl.ANY)
    dma = pltpu.SemaphoreType.DMA
    return pl.pallas_call(
        kernel,
        name="sage",
        out_shape=jax.ShapeDtypeStruct((SEEDS, HH), BF),
        in_specs=[hbm, hbm, vmem, hbm, vmem] + [hbm] * 7,
        out_specs=vmem,
        scratch_shapes=[
            pltpu.VMEM((NODE, FH), BF),
            pltpu.VMEM((2, 2 * FH, HH), BF),
            pltpu.VMEM((2, 2 * H, HH), BF),
            pltpu.VMEM((128, 16), I32),
            pltpu.VMEM((HOP, 10), I32),
            pltpu.VMEM((HOP // 128, 128), I32),
            pltpu.VMEM((HOP // 128, 128), I32),
            pltpu.VMEM((SEEDS, 5), I32),
            pltpu.VMEM((SEEDS // 128, 128), I32),
            pltpu.VMEM((SEEDS // 128, 128), I32),
            pltpu.VMEM((NP, 1, 128), I32),
            pltpu.VMEM((NZ, NP, 1, 128), I32),
            pltpu.VMEM((128, NP), I32),
            pltpu.VMEM((BLK, NODE), BF),
            pltpu.VMEM((NZ * NP, ROWS, FH), BF),
            pltpu.VMEM((NZ * NP, ROWS, FH), BF),
            pltpu.VMEM((2 * HOP, SLOTS), BF),
            pltpu.VMEM((2 * HOP, FH), F32),
            pltpu.VMEM((HOP, 10), I32),
            pltpu.VMEM((HOP, 10), I32),
            pltpu.VMEM((HOP, 10), I32),
            pltpu.VMEM((HOP, 1), I32),
            pltpu.VMEM((HOP, 1), F32),
            pltpu.VMEM((HOP, H), F32),
            pltpu.VMEM((NBLK, BLK, H), BF),
            pltpu.VMEM((NBLK, BLK, H), BF),
            pltpu.VMEM((2 * SEEDS, HOP), BF),
            pltpu.VMEM((2 * SEEDS, H), F32),
            pltpu.VMEM((SEEDS, 1), F32),
            dma((11,)),
            dma((3,)),
            dma((3,)),
            dma,
            dma,
            dma((NZ,)),
            dma((NZ,)),
            dma((NZ,)),
            dma((NZ,)),
            dma((NBLK,)),
            dma((NBLK,)),
        ],
        compiler_params=pltpu.CompilerParams(
            collective_id=0, has_side_effects=True, vmem_limit_bytes=60 * 1024 * 1024
        ),
    )(
        table,
        weight_a,
        bias_a.reshape(1, H),
        weight_b,
        bias_b.reshape(2, HH),
        requests.reshape(128, 16),
        near_a,
        self_a.reshape(HOP // 128, 128),
        count_a.reshape(HOP // 128, 128),
        near_b,
        self_b.reshape(SEEDS // 128, 128),
        count_b.reshape(SEEDS // 128, 128),
    )


def solution(mesh):
    placed = (
        P("dom", "mp"),
        P(None, "mp"),
        P(),
        P(None, "mp"),
        P(),
        P("dom", None, None),
        P("dom", None),
        P("dom"),
        P("dom"),
        P("dom", None),
        P("dom"),
        P("dom"),
    )
    return jax.shard_map(
        shards, mesh=mesh, in_specs=placed, out_specs=P("dom", "mp"), check_vma=False
    )
```

```python
import functools

import jax
import jax.numpy as jnp
from jax import lax
from jax.experimental import pallas as pl
from jax.experimental.pallas import tpu as pltpu
from jax.sharding import PartitionSpec as P

F = 768
H = 512
FH = 384
HH = 256
NX, NY, NZ = 4, 4, 8
NP = NX * NY
ROWS = 16
HOP = 1024
SLOTS = 2048
SEEDS = 256
NODE = 4096
EARLY = 28
ORDER = (0, 1, 7, 2, 6, 3, 5, 4)
BLK = 256
NBLK = HOP // BLK
MESH = pl.DeviceIdType.MESH
I32 = jnp.int32
F32 = jnp.float32
BF = jnp.bfloat16


def kernel(
    table, wa, ba, wb, bb, req, near_a, self_a, cnt_a, near_b, self_b, cnt_b,
    out,
    table_v, wa_v, wb_v, req_v, near_v, selfa_v, cnta_v, nearb_v, selfb_v, cntb_v,
    req2, zreq, tz, pick, stag, xbuf, amat, acc, lo_s, w0_s, w1_s, selfc, invc,
    part, psend, precv, bmat, accb, invb,
    lsem, wsem, wrsem, psem, prsem, zsem, zrsem, fsem, frsem, qsem, qrsem,
):
    d = lax.axis_index("dom")
    c = lax.axis_index("mp")
    x, z, y = d // (NZ * NY), (d // NY) % NZ, d % NY
    qme = x * NY + y
    mate = (d, 1 - c)

    def at_plane(m):
        tx = (x + m // NY) % NX
        ty = (y + m % NY) % NY
        return tx, ty, tx * NY + ty

    def dev(tx, tz_, ty):
        return (tx * (NZ * NY) + tz_ * NY + ty, c)

    local = []

    def bring(src, dst):
        cp = pltpu.make_async_copy(src, dst, lsem.at[len(local)])
        cp.start()
        local.append(cp)
        return cp

    c_req = bring(req, req_v)
    c_idx = [bring(near_a, near_v), bring(self_a, selfa_v), bring(cnt_a, cnta_v)]
    c_tab = bring(table, table_v)
    c_idb = [bring(near_b, nearb_v), bring(self_b, selfb_v), bring(cnt_b, cntb_v)]
    mine = pl.multiple_of(c * FH, 128)
    c_w = [
        bring(wa.at[pl.ds(mine, FH)], wa_v.at[c, pl.ds(0, FH)]),
        bring(wa.at[pl.ds(F + mine, FH)], wa_v.at[c, pl.ds(FH, FH)]),
        bring(wb, wb_v.at[c]),
    ]

    barrier = pltpu.get_barrier_semaphore()
    for m in range(1, NP):
        tx, ty, _ = at_plane(m)
        pl.semaphore_signal(barrier, inc=1, device_id=dev(tx, z, ty), device_id_type=MESH)
    for j in range(1, NZ):
        pl.semaphore_signal(barrier, inc=1, device_id=dev(x, (z + j) % NZ, y), device_id_type=MESH)
    pl.semaphore_signal(barrier, inc=1, device_id=mate, device_id_type=MESH)

    c_req.wait()
    r = req_v[...].T
    rows2 = jnp.concatenate(
        [
            jnp.concatenate([r[a * 32 + k * 4 : a * 32 + k * 4 + 4, :] for a in range(NX)], axis=0)
            for k in range(NZ)
        ],
        axis=1,
    )
    req2[...] = rows2.reshape(NP, 1, 128)

    for cp in c_idx:
        cp.wait()

    def place(s):
        kk = (((s >> 6) & 7) - z) & 7
        return (kk << 8) | ((s >> 9) << 6) | (s & 63)

    self_t = place(selfa_v[...]).T
    inv_t = (1.0 / cnta_v[...].astype(F32)).T
    filler = jnp.zeros((16 - near_v.shape[0], 128), I32)
    for g in range(HOP // 128):
        rows = pl.ds(g * 128, 128)
        selfc[rows, :] = self_t[:, g : g + 1]
        invc[rows, :] = inv_t[:, g : g + 1]
        p = place(near_v[:, rows])
        valid = lax.broadcasted_iota(I32, p.shape, 0) < cnta_v[pl.ds(g, 1), :]
        one = jnp.left_shift(jnp.ones_like(p), ((p >> 7) & 7) * 4)
        w0 = jnp.where(valid & (p < 1024), one, 0)
        w1 = jnp.where(valid & (p >= 1024), one, 0)
        for to, v in ((lo_s, p & 127), (w0_s, w0), (w1_s, w1)):
            to[rows, :] = jnp.concatenate([v, filler], axis=0).T

    pl.semaphore_wait(barrier, NP - 1 + NZ - 1 + 1)

    for m in range(1, NP):
        tx, ty, q = at_plane(m)
        pltpu.make_async_remote_copy(
            src_ref=req2.at[q], dst_ref=zreq.at[0, qme], send_sem=psem, recv_sem=prsem,
            device_id=dev(tx, z, ty), device_id_type=MESH,
        ).start()
    zreq[0, qme] = req2[qme]

    lanes = lax.broadcasted_iota(I32, (16, 128), 1)

    def build(rb, _):
        rows = pl.ds(pl.multiple_of(rb * 16, 16), 16)
        rows_s = pl.ds(pl.multiple_of(HOP + rb * 16, 16), 16)
        lo, w0, w1 = lo_s[rows, :], w0_s[rows, :], w1_s[rows, :]
        a0 = jnp.zeros((16, 128), I32)
        a1 = jnp.zeros((16, 128), I32)
        for j in range(near_v.shape[0]):
            hit = lo[:, j : j + 1] == lanes
            a0 = a0 + jnp.where(hit, w0[:, j : j + 1], 0)
            a1 = a1 + jnp.where(hit, w1[:, j : j + 1], 0)
        own = jnp.broadcast_to(selfc[rows, :], (16, 128))
        for t in range(SLOTS // 128):
            word = a0 if t < 8 else a1
            v = jnp.right_shift(word, 4 * (t % 8)) & 15
            cols = pl.ds(t * 128, 128)
            amat[rows, cols] = v.astype(F32).astype(BF)
            amat[rows_s, cols] = jnp.where(own == lanes + t * 128, 1.0, 0.0).astype(BF)
        return 0

    lax.fori_loop(0, EARLY, build, 0)

    got = pltpu.make_async_remote_copy(
        src_ref=req2.at[pl.ds(0, NP - 1)], dst_ref=zreq.at[0, pl.ds(0, NP - 1)],
        send_sem=psem, recv_sem=prsem, device_id=mate, device_id_type=MESH,
    )
    got.wait_recv()

    def z_copy(j):
        return pltpu.make_async_remote_copy(
            src_ref=zreq.at[0], dst_ref=zreq.at[(NZ - j) % NZ],
            send_sem=zsem.at[j], recv_sem=zrsem.at[(NZ - j) % NZ],
            device_id=dev(x, (z + j) % NZ, y), device_id_type=MESH,
        )

    for j in (1, 7, 2, 6, 3, 5, 4):
        z_copy(j).start()

    other = pl.multiple_of((1 - c) * FH, 128)
    w_out = []
    for i, (src, dst) in enumerate(
        (
            (wa.at[pl.ds(other, FH)], wa_v.at[c, pl.ds(0, FH)]),
            (wa.at[pl.ds(F + other, FH)], wa_v.at[c, pl.ds(FH, FH)]),
            (wb, wb_v.at[c]),
        )
    ):
        cp = pltpu.make_async_remote_copy(
            src_ref=src, dst_ref=dst, send_sem=wsem.at[i], recv_sem=wrsem.at[i],
            device_id=mate, device_id_type=MESH,
        )
        cp.start()
        w_out.append(cp)

    c_tab.wait()

    def order(i):
        return sum(k * (i == n).astype(I32) for n, k in enumerate(ORDER))

    def feature_send(k, m):
        tx, ty, q = at_plane(m)
        kk = (NZ - k) % NZ
        return pltpu.make_async_remote_copy(
            src_ref=stag.at[k * NP + q], dst_ref=xbuf.at[kk * NP + qme],
            send_sem=fsem.at[k], recv_sem=frsem.at[kk],
            device_id=dev(tx, (z + k) % NZ, ty), device_id_type=MESH,
        )

    def gather(k):
        tz[...] = zreq[k].reshape(NP, 128).T
        idx = tz[pl.ds(pl.multiple_of(z * 16, 16), 16), :]
        for q in range(NP):
            want = jnp.broadcast_to(idx[:, q : q + 1], (16, 128))
            for t in range(NODE // 128):
                pick[pl.ds(q * 16, 16), pl.ds(t * 128, 128)] = jnp.where(
                    want == lanes + t * 128, 1.0, 0.0
                ).astype(BF)
        rows = jnp.dot(pick[...], table_v[...], preferred_element_type=F32)
        stag[pl.ds(k * NP, NP)] = rows.astype(BF).reshape(NP, ROWS, FH)

    def serve(i, _):
        k = order(i)

        @pl.when(i > 0)
        def _():
            pltpu.make_async_remote_copy(
                src_ref=zreq.at[0], dst_ref=zreq.at[k], send_sem=zsem.at[0], recv_sem=zrsem.at[k],
                device_id=mate, device_id_type=MESH,
            ).wait_recv()

        gather(k)

        @pl.when(i > 0)
        def _():
            feature_send(k, 0).start()

        for m in range(1, NP):
            feature_send(k, m).start()
        return 0

    lax.fori_loop(0, NZ, serve, 0)
    lax.fori_loop(EARLY, HOP // 16, build, 0)
    xbuf[qme] = stag[qme]

    for cp in c_idb:
        cp.wait()
    selfb_t = selfb_v[...].T
    invb_t = (1.0 / cntb_v[...].astype(F32)).T
    for g in range(SEEDS // 128):
        cols = pl.ds(g * 128, 128)
        invb[cols, :] = invb_t[:, g : g + 1]
        nb = nearb_v[:, cols]
        nb = jnp.where(lax.broadcasted_iota(I32, nb.shape, 0) < cntb_v[pl.ds(g, 1), :], nb, -1)
        nb = jnp.concatenate([nb, jnp.full((8 - nb.shape[0], 128), -1, I32)], axis=0).T
        sb = selfb_t[:, g : g + 1]
        for s in range(8):
            for t in range(HOP // 128):
                tot = jnp.zeros((16, 128), F32)
                for j in range(nearb_v.shape[0]):
                    tot = tot + jnp.where(nb[s * 16 : s * 16 + 16, j : j + 1] == lanes + t * 128, 1.0, 0.0)
                bmat[pl.ds(g * 128 + s * 16, 16), pl.ds(t * 128, 128)] = tot.astype(BF)
                hit = sb[s * 16 : s * 16 + 16] == lanes + t * 128
                bmat[pl.ds(SEEDS + g * 128 + s * 16, 16), pl.ds(t * 128, 128)] = jnp.where(
                    hit, 1.0, 0.0
                ).astype(BF)

    def add_up(k, first):
        xk = xbuf[pl.ds(k * NP, NP)].reshape(BLK, FH)

        def rows_of(b, _):
            rows = pl.ds(pl.multiple_of(b * 512, 512), 512)
            cols = pl.ds(pl.multiple_of(k * BLK, BLK), BLK)
            tot = jnp.dot(amat[rows, cols], xk, preferred_element_type=F32)
            if first:
                acc[rows, :] = tot
            else:
                acc[rows, :] += tot
            return 0

        lax.fori_loop(0, SLOTS // 512, rows_of, 0)

    def arrived(k, n):
        pltpu.make_async_remote_copy(
            src_ref=stag.at[pl.ds(0, n)], dst_ref=xbuf.at[pl.ds(k * NP, n)],
            send_sem=fsem.at[0], recv_sem=frsem.at[k], device_id=mate, device_id_type=MESH,
        ).wait_recv()

    arrived(0, NP - 1)
    add_up(0, True)

    def collect(i, _):
        k = (NZ - order(i)) % NZ
        arrived(k, NP)
        add_up(k, False)
        return 0

    lax.fori_loop(1, NZ, collect, 0)

    for cp in c_w:
        cp.wait()
    for cp in w_out:
        cp.wait_recv()

    def half_copy(b):
        return pltpu.make_async_remote_copy(
            src_ref=psend.at[b], dst_ref=precv.at[b], send_sem=qsem.at[b], recv_sem=qrsem.at[b],
            device_id=mate, device_id_type=MESH,
        )

    for b in range(NBLK):
        rows = pl.ds(b * BLK, BLK)
        own = acc[pl.ds(HOP + b * BLK, BLK), :].astype(BF)
        mean = (acc[rows, :] * invc[rows, :]).astype(BF)
        both = jnp.concatenate([own, mean], axis=1)
        for h in range(2):
            v = jnp.dot(both, wa_v[h], preferred_element_type=F32)
            part[rows, pl.ds(h * HH, HH)] = v
            psend[b, :, pl.ds(h * HH, HH)] = v.astype(BF)
        half_copy(b).start()

    for b in range(NBLK):
        rows = pl.ds(b * BLK, BLK)
        half_copy(b).wait_recv()
        v = part[rows, :] + precv[b].astype(F32) + ba[...]
        hid = jnp.maximum(v, 0.0).astype(BF)
        tot = jnp.dot(bmat[:, pl.ds(b * BLK, BLK)], hid, preferred_element_type=F32)
        if b == 0:
            accb[...] = tot
        else:
            accb[...] += tot

    own = accb[pl.ds(SEEDS, SEEDS), :].astype(BF)
    mean = (accb[pl.ds(0, SEEDS), :] * invb[...]).astype(BF)
    both = jnp.concatenate([own, mean], axis=1)

    def state_of(h):
        v = jnp.dot(both, wb_v[h], preferred_element_type=F32) + bb[:, pl.ds(pl.multiple_of(h * HH, HH), HH)]
        return jnp.maximum(v, 0.0)

    s0 = state_of(c)
    s1 = state_of(1 - c)
    squares = jnp.sum(s0 * s0, axis=1, keepdims=True) + jnp.sum(s1 * s1, axis=1, keepdims=True)
    out[...] = (s0 * jnp.sqrt(jnp.float32(H)) / jnp.sqrt(squares + H)).astype(BF)

    got.wait_send()
    for j in range(1, NZ):
        z_copy(j).wait_send()
    for cp in w_out:
        cp.wait_send()
    for k in range(NZ):
        n = NP - 1 if k == 0 else NP
        pltpu.make_async_remote_copy(
            src_ref=stag.at[pl.ds(k * NP, n)], dst_ref=xbuf.at[pl.ds(0, n)],
            send_sem=fsem.at[k], recv_sem=frsem.at[0], device_id=mate, device_id_type=MESH,
        ).wait_send()
    for b in range(NBLK):
        half_copy(b).wait_send()


def shards(
    table, weight_a, bias_a, weight_b, bias_b, requests,
    near_a, self_a, count_a, near_b, self_b, count_b,
):
    vmem = pl.BlockSpec(memory_space=pltpu.VMEM)
    hbm = pl.BlockSpec(memory_space=pl.ANY)
    dma = pltpu.SemaphoreType.DMA
    return pl.pallas_call(
        kernel,
        name="sage",
        out_shape=jax.ShapeDtypeStruct((SEEDS, HH), BF),
        in_specs=[hbm, hbm, vmem, hbm, vmem] + [hbm] * 7,
        out_specs=vmem,
        scratch_shapes=[
            pltpu.VMEM((NODE, FH), BF),
            pltpu.VMEM((2, 2 * FH, HH), BF),
            pltpu.VMEM((2, 2 * H, HH), BF),
            pltpu.VMEM((16, 128), I32),
            pltpu.VMEM((10, HOP), I32),
            pltpu.VMEM((HOP // 128, 128), I32),
            pltpu.VMEM((HOP // 128, 128), I32),
            pltpu.VMEM((5, SEEDS), I32),
            pltpu.VMEM((SEEDS // 128, 128), I32),
            pltpu.VMEM((SEEDS // 128, 128), I32),
            pltpu.VMEM((NP, 1, 128), I32),
            pltpu.VMEM((NZ, NP, 1, 128), I32),
            pltpu.VMEM((128, NP), I32),
            pltpu.VMEM((BLK, NODE), BF),
            pltpu.VMEM((NZ * NP, ROWS, FH), BF),
            pltpu.VMEM((NZ * NP, ROWS, FH), BF),
            pltpu.VMEM((2 * HOP, SLOTS), BF),
            pltpu.VMEM((2 * HOP, FH), F32),
            pltpu.VMEM((HOP, 16), I32),
            pltpu.VMEM((HOP, 16), I32),
            pltpu.VMEM((HOP, 16), I32),
            pltpu.VMEM((HOP, 1), I32),
            pltpu.VMEM((HOP, 1), F32),
            pltpu.VMEM((HOP, H), F32),
            pltpu.VMEM((NBLK, BLK, H), BF),
            pltpu.VMEM((NBLK, BLK, H), BF),
            pltpu.VMEM((2 * SEEDS, HOP), BF),
            pltpu.VMEM((2 * SEEDS, H), F32),
            pltpu.VMEM((SEEDS, 1), F32),
            dma((11,)),
            dma((3,)),
            dma((3,)),
            dma,
            dma,
            dma((NZ,)),
            dma((NZ,)),
            dma((NZ,)),
            dma((NZ,)),
            dma((NBLK,)),
            dma((NBLK,)),
        ],
        compiler_params=pltpu.CompilerParams(
            collective_id=0, has_side_effects=True, vmem_limit_bytes=60 * 1024 * 1024
        ),
    )(
        table,
        weight_a,
        bias_a.reshape(1, H),
        weight_b,
        bias_b.reshape(1, H),
        jnp.swapaxes(requests[0], 0, 1),
        near_a.T,
        self_a.reshape(HOP // 128, 128),
        count_a.reshape(HOP // 128, 128),
        near_b.T,
        self_b.reshape(SEEDS // 128, 128),
        count_b.reshape(SEEDS // 128, 128),
    )


def solution(mesh):
    placed = (
        P("dom", "mp"),
        P(None, "mp"),
        P(),
        P(None, "mp"),
        P(),
        P("dom", None, None),
        P("dom", None),
        P("dom"),
        P("dom"),
        P("dom", None),
        P("dom"),
        P("dom"),
    )
    return jax.shard_map(
        shards, mesh=mesh, in_specs=placed, out_specs=P("dom", "mp"), check_vma=False
    )
```

```python
import functools

import jax
import jax.numpy as jnp
from jax import lax
from jax.experimental import pallas as pl
from jax.experimental.pallas import tpu as pltpu
from jax.sharding import PartitionSpec as P

F = 768
H = 512
FH = 384
HH = 256
NX, NY, NZ = 4, 4, 8
NP = NX * NY
ROWS = 16
HOP = 1024
SLOTS = 2048
SEEDS = 256
NODE = 4096
ORDER = (0, 1, 7, 2, 6, 3, 5, 4)
BLK = 256
NBLK = HOP // BLK
MESH = pl.DeviceIdType.MESH
I32 = jnp.int32
F32 = jnp.float32
BF = jnp.bfloat16


def kernel(
    table, wa, ba, wb, bb, req, near_a, self_a, cnt_a, near_b, self_b, cnt_b,
    out,
    table_v, wa_v, wb_v, ba_v, bb_v, req_v, near_v, selfa_v, cnta_v, nearb_v, selfb_v, cntb_v,
    req2, zreq, tz, pick, stag, xbuf, amat, acc, lo_s, w0_s, w1_s, selfc, invc,
    part, psend, precv, bmat, accb, invb,
    lsem, wsem, wrsem, psem, prsem, zsem, zrsem, fsem, frsem, qsem, qrsem,
):
    d = lax.axis_index("dom")
    c = lax.axis_index("mp")
    x, z, y = d // (NZ * NY), (d // NY) % NZ, d % NY
    qme = x * NY + y
    mate = (d, 1 - c)

    def at_plane(m):
        tx = (x + m // NY) % NX
        ty = (y + m % NY) % NY
        return tx, ty, tx * NY + ty

    def dev(tx, tz_, ty):
        return (tx * (NZ * NY) + tz_ * NY + ty, c)

    local = []

    def bring(src, dst):
        cp = pltpu.make_async_copy(src, dst, lsem.at[len(local)])
        cp.start()
        local.append(cp)
        return cp

    c_req = bring(req, req_v)
    c_idx = [bring(near_a, near_v), bring(self_a, selfa_v), bring(cnt_a, cnta_v)]
    c_tab = bring(table, table_v)
    c_idb = [bring(near_b, nearb_v), bring(self_b, selfb_v), bring(cnt_b, cntb_v)]
    c_bias = [bring(ba, ba_v), bring(bb, bb_v)]
    mine = pl.multiple_of(c * FH, 128)
    c_w = [
        bring(wa.at[pl.ds(mine, FH)], wa_v.at[c, pl.ds(0, FH)]),
        bring(wa.at[pl.ds(F + mine, FH)], wa_v.at[c, pl.ds(FH, FH)]),
        bring(wb, wb_v.at[c]),
    ]

    barrier = pltpu.get_barrier_semaphore()
    for m in range(1, NP):
        tx, ty, _ = at_plane(m)
        pl.semaphore_signal(barrier, inc=1, device_id=dev(tx, z, ty), device_id_type=MESH)
    for j in range(1, NZ):
        pl.semaphore_signal(barrier, inc=1, device_id=dev(x, (z + j) % NZ, y), device_id_type=MESH)
    pl.semaphore_signal(barrier, inc=1, device_id=mate, device_id_type=MESH)

    c_req.wait()
    r = req_v[...].T
    rows2 = jnp.concatenate(
        [
            jnp.concatenate([r[a * 32 + k * 4 : a * 32 + k * 4 + 4, :] for a in range(NX)], axis=0)
            for k in range(NZ)
        ],
        axis=1,
    )
    req2[...] = rows2.reshape(NP, 1, 128)

    pl.semaphore_wait(barrier, NP - 1 + NZ - 1 + 1)

    for m in range(1, NP):
        tx, ty, q = at_plane(m)
        pltpu.make_async_remote_copy(
            src_ref=req2.at[q], dst_ref=zreq.at[0, qme], send_sem=psem, recv_sem=prsem,
            device_id=dev(tx, z, ty), device_id_type=MESH,
        ).start()
    zreq[0, qme] = req2[qme]

    lanes = lax.broadcasted_iota(I32, (16, 128), 1)

    got = pltpu.make_async_remote_copy(
        src_ref=req2.at[pl.ds(0, NP - 1)], dst_ref=zreq.at[0, pl.ds(0, NP - 1)],
        send_sem=psem, recv_sem=prsem, device_id=mate, device_id_type=MESH,
    )
    got.wait_recv()

    def z_copy(j):
        return pltpu.make_async_remote_copy(
            src_ref=zreq.at[0], dst_ref=zreq.at[(NZ - j) % NZ],
            send_sem=zsem.at[j], recv_sem=zrsem.at[(NZ - j) % NZ],
            device_id=dev(x, (z + j) % NZ, y), device_id_type=MESH,
        )

    for j in (1, 7, 2, 6, 3, 5, 4):
        z_copy(j).start()

    other = pl.multiple_of((1 - c) * FH, 128)
    w_out = []
    for i, (src, dst) in enumerate(
        (
            (wa.at[pl.ds(other, FH)], wa_v.at[c, pl.ds(0, FH)]),
            (wa.at[pl.ds(F + other, FH)], wa_v.at[c, pl.ds(FH, FH)]),
            (wb, wb_v.at[c]),
        )
    ):
        cp = pltpu.make_async_remote_copy(
            src_ref=src, dst_ref=dst, send_sem=wsem.at[i], recv_sem=wrsem.at[i],
            device_id=mate, device_id_type=MESH,
        )
        cp.start()
        w_out.append(cp)

    c_tab.wait()

    def order(i):
        return sum(k * (i == n).astype(I32) for n, k in enumerate(ORDER))

    def feature_send(k, m):
        tx, ty, q = at_plane(m)
        kk = (NZ - k) % NZ
        return pltpu.make_async_remote_copy(
            src_ref=stag.at[k * NP + q], dst_ref=xbuf.at[kk * NP + qme],
            send_sem=fsem.at[k], recv_sem=frsem.at[kk],
            device_id=dev(tx, (z + k) % NZ, ty), device_id_type=MESH,
        )

    def gather(k):
        tz[...] = zreq[k].reshape(NP, 128).T
        idx = tz[pl.ds(pl.multiple_of(z * 16, 16), 16), :]
        for q in range(NP):
            want = jnp.broadcast_to(idx[:, q : q + 1], (16, 128))
            for t in range(NODE // 128):
                pick[pl.ds(q * 16, 16), pl.ds(t * 128, 128)] = jnp.where(
                    want == lanes + t * 128, 1.0, 0.0
                ).astype(BF)
        rows = jnp.dot(pick[...], table_v[...], preferred_element_type=F32)
        stag[pl.ds(k * NP, NP)] = rows.astype(BF).reshape(NP, ROWS, FH)

    def serve(i, _):
        k = order(i)

        @pl.when(k > 0)
        def _():
            pltpu.make_async_remote_copy(
                src_ref=zreq.at[0], dst_ref=zreq.at[k], send_sem=zsem.at[0], recv_sem=zrsem.at[k],
                device_id=mate, device_id_type=MESH,
            ).wait_recv()

        gather(k)

        @pl.when(k > 0)
        def _():
            feature_send(k, 0).start()

        for m in range(1, NP):
            feature_send(k, m).start()
        return 0

    lax.fori_loop(0, NZ, serve, 0)
    xbuf[qme] = stag[qme]

    for cp in c_idx:
        cp.wait()

    def place(s):
        kk = (((s >> 6) & 7) - z) & 7
        return (kk << 8) | ((s >> 9) << 6) | (s & 63)

    self_t = place(selfa_v[...]).T
    inv_t = (1.0 / cnta_v[...].astype(F32)).T
    filler = jnp.zeros((16 - near_v.shape[0], 128), I32)
    for g in range(HOP // 128):
        rows = pl.ds(g * 128, 128)
        selfc[rows, :] = self_t[:, g : g + 1]
        invc[rows, :] = inv_t[:, g : g + 1]
        p = place(near_v[:, rows])
        valid = lax.broadcasted_iota(I32, p.shape, 0) < cnta_v[pl.ds(g, 1), :]
        one = jnp.left_shift(jnp.ones_like(p), ((p >> 7) & 7) * 4)
        w0 = jnp.where(valid & (p < 1024), one, 0)
        w1 = jnp.where(valid & (p >= 1024), one, 0)
        for to, v in ((lo_s, p & 127), (w0_s, w0), (w1_s, w1)):
            to[rows, :] = jnp.concatenate([v, filler], axis=0).T

    def build(rb, _):
        rows = pl.ds(pl.multiple_of(rb * 16, 16), 16)
        rows_s = pl.ds(pl.multiple_of(HOP + rb * 16, 16), 16)
        lo, w0, w1 = lo_s[rows, :], w0_s[rows, :], w1_s[rows, :]
        a0 = jnp.zeros((16, 128), I32)
        a1 = jnp.zeros((16, 128), I32)
        for j in range(near_v.shape[0]):
            hit = lo[:, j : j + 1] == lanes
            a0 = a0 + jnp.where(hit, w0[:, j : j + 1], 0)
            a1 = a1 + jnp.where(hit, w1[:, j : j + 1], 0)
        own = jnp.broadcast_to(selfc[rows, :], (16, 128))
        for t in range(SLOTS // 128):
            word = a0 if t < 8 else a1
            v = jnp.right_shift(word, 4 * (t % 8)) & 15
            cols = pl.ds(t * 128, 128)
            amat[rows, cols] = v.astype(F32).astype(BF)
            amat[rows_s, cols] = jnp.where(own == lanes + t * 128, 1.0, 0.0).astype(BF)
        return 0

    lax.fori_loop(0, HOP // 16, build, 0)

    for cp in c_idb:
        cp.wait()
    selfb_t = selfb_v[...].T
    invb_t = (1.0 / cntb_v[...].astype(F32)).T
    for g in range(SEEDS // 128):
        cols = pl.ds(g * 128, 128)
        invb[cols, :] = invb_t[:, g : g + 1]
        nb = nearb_v[:, cols]
        nb = jnp.where(lax.broadcasted_iota(I32, nb.shape, 0) < cntb_v[pl.ds(g, 1), :], nb, -1)
        nb = jnp.concatenate([nb, jnp.full((8 - nb.shape[0], 128), -1, I32)], axis=0).T
        sb = selfb_t[:, g : g + 1]
        for s in range(8):
            for t in range(HOP // 128):
                tot = jnp.zeros((16, 128), F32)
                for j in range(nearb_v.shape[0]):
                    tot = tot + jnp.where(nb[s * 16 : s * 16 + 16, j : j + 1] == lanes + t * 128, 1.0, 0.0)
                bmat[pl.ds(g * 128 + s * 16, 16), pl.ds(t * 128, 128)] = tot.astype(BF)
                hit = sb[s * 16 : s * 16 + 16] == lanes + t * 128
                bmat[pl.ds(SEEDS + g * 128 + s * 16, 16), pl.ds(t * 128, 128)] = jnp.where(
                    hit, 1.0, 0.0
                ).astype(BF)

    def add_up(k, first):
        xk = xbuf[pl.ds(k * NP, NP)].reshape(BLK, FH)

        def rows_of(b, _):
            rows = pl.ds(pl.multiple_of(b * 512, 512), 512)
            cols = pl.ds(pl.multiple_of(k * BLK, BLK), BLK)
            tot = jnp.dot(amat[rows, cols], xk, preferred_element_type=F32)
            if first:
                acc[rows, :] = tot
            else:
                acc[rows, :] += tot
            return 0

        lax.fori_loop(0, SLOTS // 512, rows_of, 0)

    def arrived(k, n):
        pltpu.make_async_remote_copy(
            src_ref=stag.at[pl.ds(0, n)], dst_ref=xbuf.at[pl.ds(k * NP, n)],
            send_sem=fsem.at[0], recv_sem=frsem.at[k], device_id=mate, device_id_type=MESH,
        ).wait_recv()

    for i in range(NZ):
        k = (NZ - ORDER[i]) % NZ
        arrived(k, NP if k else NP - 1)
        add_up(k, i == 0)

    for cp in c_bias + c_w:
        cp.wait()
    for cp in w_out:
        cp.wait_recv()

    def half_copy(b):
        return pltpu.make_async_remote_copy(
            src_ref=psend.at[b], dst_ref=precv.at[b], send_sem=qsem.at[b], recv_sem=qrsem.at[b],
            device_id=mate, device_id_type=MESH,
        )

    for b in range(NBLK):
        rows = pl.ds(b * BLK, BLK)
        own = acc[pl.ds(HOP + b * BLK, BLK), :].astype(BF)
        mean = (acc[rows, :] * invc[rows, :]).astype(BF)
        both = jnp.concatenate([own, mean], axis=1)
        for h in range(2):
            v = jnp.dot(both, wa_v[h], preferred_element_type=F32)
            part[rows, pl.ds(h * HH, HH)] = v
            psend[b, :, pl.ds(h * HH, HH)] = v.astype(BF)
        half_copy(b).start()

    for b in range(NBLK):
        rows = pl.ds(b * BLK, BLK)
        half_copy(b).wait_recv()
        v = part[rows, :] + precv[b].astype(F32) + ba_v[...]
        hid = jnp.maximum(v, 0.0).astype(BF)
        tot = jnp.dot(bmat[:, pl.ds(b * BLK, BLK)], hid, preferred_element_type=F32)
        if b == 0:
            accb[...] = tot
        else:
            accb[...] += tot

    own = accb[pl.ds(SEEDS, SEEDS), :].astype(BF)
    mean = (accb[pl.ds(0, SEEDS), :] * invb[...]).astype(BF)
    both = jnp.concatenate([own, mean], axis=1)

    def state_of(h):
        v = jnp.dot(both, wb_v[h], preferred_element_type=F32) + bb_v[:, pl.ds(pl.multiple_of(h * HH, HH), HH)]
        return jnp.maximum(v, 0.0)

    s0 = state_of(c)
    s1 = state_of(1 - c)
    squares = jnp.sum(s0 * s0, axis=1, keepdims=True) + jnp.sum(s1 * s1, axis=1, keepdims=True)
    out[...] = (s0 * jnp.sqrt(jnp.float32(H)) / jnp.sqrt(squares + H)).astype(BF)

    got.wait_send()
    for j in range(1, NZ):
        z_copy(j).wait_send()
    for cp in w_out:
        cp.wait_send()
    for k in range(NZ):
        n = NP - 1 if k == 0 else NP
        pltpu.make_async_remote_copy(
            src_ref=stag.at[pl.ds(k * NP, n)], dst_ref=xbuf.at[pl.ds(0, n)],
            send_sem=fsem.at[k], recv_sem=frsem.at[0], device_id=mate, device_id_type=MESH,
        ).wait_send()
    for b in range(NBLK):
        half_copy(b).wait_send()


def shards(
    table, weight_a, bias_a, weight_b, bias_b, requests,
    near_a, self_a, count_a, near_b, self_b, count_b,
):
    vmem = pl.BlockSpec(memory_space=pltpu.VMEM)
    hbm = pl.BlockSpec(memory_space=pl.ANY)
    dma = pltpu.SemaphoreType.DMA
    return pl.pallas_call(
        kernel,
        name="sage",
        out_shape=jax.ShapeDtypeStruct((SEEDS, HH), BF),
        in_specs=[hbm] * 12,
        out_specs=vmem,
        scratch_shapes=[
            pltpu.VMEM((NODE, FH), BF),
            pltpu.VMEM((2, 2 * FH, HH), BF),
            pltpu.VMEM((2, 2 * H, HH), BF),
            pltpu.VMEM((1, H), F32),
            pltpu.VMEM((1, H), F32),
            pltpu.VMEM((16, 128), I32),
            pltpu.VMEM((10, HOP), I32),
            pltpu.VMEM((HOP // 128, 128), I32),
            pltpu.VMEM((HOP // 128, 128), I32),
            pltpu.VMEM((5, SEEDS), I32),
            pltpu.VMEM((SEEDS // 128, 128), I32),
            pltpu.VMEM((SEEDS // 128, 128), I32),
            pltpu.VMEM((NP, 1, 128), I32),
            pltpu.VMEM((NZ, NP, 1, 128), I32),
            pltpu.VMEM((128, NP), I32),
            pltpu.VMEM((BLK, NODE), BF),
            pltpu.VMEM((NZ * NP, ROWS, FH), BF),
            pltpu.VMEM((NZ * NP, ROWS, FH), BF),
            pltpu.VMEM((2 * HOP, SLOTS), BF),
            pltpu.VMEM((2 * HOP, FH), F32),
            pltpu.VMEM((HOP, 16), I32),
            pltpu.VMEM((HOP, 16), I32),
            pltpu.VMEM((HOP, 16), I32),
            pltpu.VMEM((HOP, 1), I32),
            pltpu.VMEM((HOP, 1), F32),
            pltpu.VMEM((HOP, H), F32),
            pltpu.VMEM((NBLK, BLK, H), BF),
            pltpu.VMEM((NBLK, BLK, H), BF),
            pltpu.VMEM((2 * SEEDS, HOP), BF),
            pltpu.VMEM((2 * SEEDS, H), F32),
            pltpu.VMEM((SEEDS, 1), F32),
            dma((13,)),
            dma((3,)),
            dma((3,)),
            dma,
            dma,
            dma((NZ,)),
            dma((NZ,)),
            dma((NZ,)),
            dma((NZ,)),
            dma((NBLK,)),
            dma((NBLK,)),
        ],
        compiler_params=pltpu.CompilerParams(
            collective_id=0, has_side_effects=True, vmem_limit_bytes=50000 * 1024
        ),
    )(
        *(
            pltpu.with_memory_space_constraint(v, pltpu.HBM)
            for v in (
        table,
        weight_a,
        bias_a.reshape(1, H),
        weight_b,
        bias_b.reshape(1, H),
        jnp.swapaxes(requests[0], 0, 1),
        near_a.T,
        self_a.reshape(HOP // 128, 128),
        count_a.reshape(HOP // 128, 128),
        near_b.T,
        self_b.reshape(SEEDS // 128, 128),
        count_b.reshape(SEEDS // 128, 128),
            )
        )
    )


def solution(mesh):
    placed = (
        P("dom", "mp"),
        P(None, "mp"),
        P(),
        P(None, "mp"),
        P(),
        P("dom", None, None),
        P("dom", None),
        P("dom"),
        P("dom"),
        P("dom", None),
        P("dom"),
        P("dom"),
    )
    return jax.shard_map(
        shards, mesh=mesh, in_specs=placed, out_specs=P("dom", "mp"), check_vma=False
    )
```

```python
import functools

import jax
import jax.numpy as jnp
from jax import lax
from jax.experimental import pallas as pl
from jax.experimental.pallas import tpu as pltpu
from jax.sharding import PartitionSpec as P

F = 768
H = 512
FH = 384
HH = 256
NX, NY, NZ = 4, 4, 8
NP = NX * NY
ROWS = 16
HOP = 1024
SLOTS = 2048
SEEDS = 256
NODE = 4096
OFFSET = (
    (0, 0), (0, 2), (0, 1), (0, 3), (1, 0), (3, 0), (1, 1), (3, 3),
    (1, 3), (3, 1), (2, 0), (2, 2), (1, 2), (3, 2), (2, 1), (2, 3),
)
BACK = tuple(OFFSET.index(((4 - a) % 4, (4 - b) % 4)) for a, b in OFFSET)
SERVE = (0, 2, 3, 4, 5, 1, 6, 7, 8, 9, 10, 12, 13, 14, 15, 11)
PAIRS = (1, 2, 0, 3, 4, 6, 7, 5)
BLK = 256
NBLK = HOP // BLK
MESH = pl.DeviceIdType.MESH
I32 = jnp.int32
F32 = jnp.float32
BF = jnp.bfloat16


def look(values, i):
    return sum(v * (i == n).astype(I32) for n, v in enumerate(values) if v)


def kernel(
    table, wa, ba, wb, bb, req, near_a, self_a, cnt_a, near_b, self_b, cnt_b,
    out,
    table_v, wa_v, wb_v, ba_v, bb_v, req_v, near_v, selfa_v, cnta_v, nearb_v, selfb_v, cntb_v,
    req_t, req2, zreq, preq, tz, pick, stag, xbuf, amat, acc, lo_s, w0_s, w1_s, selfc, invc,
    part, psend, precv, bmat, accb, invb,
    lsem, wsem, wrsem, psem, prsem, zsem, zrsem, fsem, frsem, qsem, qrsem,
):
    d = lax.axis_index("dom")
    c = lax.axis_index("mp")
    x, z, y = d // (NZ * NY), (d // NY) % NZ, d % NY
    qme = x * NY + y
    mate = (d, 1 - c)

    def at_plane(n):
        a, b = OFFSET[n] if isinstance(n, int) else (look([o[0] for o in OFFSET], n), look([o[1] for o in OFFSET], n))
        tx, ty = (x + a) % NX, (y + b) % NY
        return tx, ty, tx * NY + ty

    def dev(tx, tz_, ty):
        return (tx * (NZ * NY) + tz_ * NY + ty, c)

    local = []

    def bring(src, dst):
        cp = pltpu.make_async_copy(src, dst, lsem.at[len(local)])
        cp.start()
        local.append(cp)
        return cp

    c_req = bring(req, req_v)
    c_idx = [bring(near_a, near_v), bring(self_a, selfa_v), bring(cnt_a, cnta_v)]
    c_tab = bring(table, table_v)
    c_idb = [bring(near_b, nearb_v), bring(self_b, selfb_v), bring(cnt_b, cntb_v)]
    c_bias = [bring(ba, ba_v), bring(bb, bb_v)]
    mine = pl.multiple_of(c * FH, 128)
    c_w = [
        bring(wa.at[pl.ds(mine, FH)], wa_v.at[c, pl.ds(0, FH)]),
        bring(wa.at[pl.ds(F + mine, FH)], wa_v.at[c, pl.ds(FH, FH)]),
        bring(wb, wb_v.at[c]),
    ]

    barrier = pltpu.get_barrier_semaphore()
    for m in range(1, NP):
        tx, ty, _ = at_plane(m)
        pl.semaphore_signal(barrier, inc=1, device_id=dev(tx, z, ty), device_id_type=MESH)
    for j in range(1, NZ):
        pl.semaphore_signal(barrier, inc=1, device_id=dev(x, (z + j) % NZ, y), device_id_type=MESH)
    pl.semaphore_signal(barrier, inc=1, device_id=mate, device_id_type=MESH)

    c_req.wait()
    req_t[...] = req_v[...].T
    for h in range(2):
        req2[h] = jnp.concatenate(
            [
                req_t[pl.ds((q // NY) * 32 + q % NY, NZ, stride=NY), :]
                for q in range(h * 8, h * 8 + 8)
            ],
            axis=1,
        ).reshape(NZ, 1, 128)

    pl.semaphore_wait(barrier, NP - 1 + NZ - 1 + 1)

    for j in (4, 3, 5, 2, 6, 1, 7):
        pltpu.make_async_remote_copy(
            src_ref=req2.at[:, (z + j) % NZ], dst_ref=zreq.at[:, NZ - j], send_sem=zsem, recv_sem=zrsem,
            device_id=dev(x, (z + j) % NZ, y), device_id_type=MESH,
        ).start()
    zreq[:, 0] = req2[:, z]

    lanes = lax.broadcasted_iota(I32, (16, 128), 1)

    got = pltpu.make_async_remote_copy(
        src_ref=req2.at[:, pl.ds(0, NZ - 1)], dst_ref=zreq.at[:, pl.ds(0, NZ - 1)],
        send_sem=zsem, recv_sem=zrsem, device_id=mate, device_id_type=MESH,
    )
    got.wait_recv()

    def plane_copy(n):
        tx, ty, q = at_plane(n)
        return pltpu.make_async_remote_copy(
            src_ref=zreq.at[q // 8], dst_ref=preq.at[BACK[n]],
            send_sem=psem.at[n], recv_sem=prsem.at[BACK[n]],
            device_id=dev(tx, z, ty), device_id_type=MESH,
        )

    for n in SERVE[1:]:
        plane_copy(n).start()
    preq[0] = zreq[qme // 8]

    other = pl.multiple_of((1 - c) * FH, 128)
    w_out = []
    for i, (src, dst) in enumerate(
        (
            (wa.at[pl.ds(other, FH)], wa_v.at[c, pl.ds(0, FH)]),
            (wa.at[pl.ds(F + other, FH)], wa_v.at[c, pl.ds(FH, FH)]),
            (wb, wb_v.at[c]),
        )
    ):
        cp = pltpu.make_async_remote_copy(
            src_ref=src, dst_ref=dst, send_sem=wsem.at[i], recv_sem=wrsem.at[i],
            device_id=mate, device_id_type=MESH,
        )
        cp.start()
        w_out.append(cp)

    c_tab.wait()

    def feature_send(n, j):
        tx, ty, _ = at_plane(n)
        back = look(BACK, n)
        return pltpu.make_async_remote_copy(
            src_ref=stag.at[n * NZ + j], dst_ref=xbuf.at[back * NZ + (NZ - j) % NZ],
            send_sem=fsem.at[n // 2], recv_sem=frsem.at[back // 2],
            device_id=dev(tx, (z + j) % NZ, ty), device_id_type=MESH,
        )

    def gather(n):
        tz[...] = preq[n].reshape(NZ, 128).T
        idx = tz[pl.ds(pl.multiple_of((qme % 8) * 16, 16), 16), :]
        for j in range(NZ):
            want = jnp.broadcast_to(idx[:, j : j + 1], (16, 128))
            for t in range(NODE // 128):
                pick[pl.ds(j * 16, 16), pl.ds(t * 128, 128)] = jnp.where(
                    want == lanes + t * 128, 1.0, 0.0
                ).astype(BF)
        rows = jnp.dot(pick[...], table_v[...], preferred_element_type=F32)
        stag[pl.ds(n * NZ, NZ)] = rows.astype(BF).reshape(NZ, ROWS, FH)

    def serve(i, _):
        n = look(SERVE, i)

        @pl.when(n > 0)
        def _():
            pltpu.make_async_remote_copy(
                src_ref=zreq.at[0], dst_ref=preq.at[n], send_sem=psem.at[0], recv_sem=prsem.at[n],
                device_id=mate, device_id_type=MESH,
            ).wait_recv()

        gather(n)
        for j in (4, 3, 5, 2, 6, 1, 7):
            feature_send(n, j).start()

        @pl.when(n > 0)
        def _():
            feature_send(n, 0).start()

        return 0

    lax.fori_loop(0, NP, serve, 0)
    xbuf[0] = stag[0]

    for cp in c_idx:
        cp.wait()

    def place(s):
        kk = (((s >> 6) & 7) - z) & 7
        m = ((((s >> 9) - x) & 3) << 2) | ((((s >> 4) & 3) - y) & 3)
        rank = sum(jnp.where(m == a * NY + b, n, 0) for n, (a, b) in enumerate(OFFSET) if n)
        return (rank << 7) | (kk << 4) | (s & 15)

    self_t = place(selfa_v[...]).T
    inv_t = (1.0 / cnta_v[...].astype(F32)).T
    filler = jnp.zeros((16 - near_v.shape[0], 128), I32)
    for g in range(HOP // 128):
        rows = pl.ds(g * 128, 128)
        selfc[rows, :] = self_t[:, g : g + 1]
        invc[rows, :] = inv_t[:, g : g + 1]
        p = place(near_v[:, rows])
        valid = lax.broadcasted_iota(I32, p.shape, 0) < cnta_v[pl.ds(g, 1), :]
        one = jnp.left_shift(jnp.ones_like(p), ((p >> 7) & 7) * 4)
        w0 = jnp.where(valid & (p < 1024), one, 0)
        w1 = jnp.where(valid & (p >= 1024), one, 0)
        for to, v in ((lo_s, p & 127), (w0_s, w0), (w1_s, w1)):
            to[rows, :] = jnp.concatenate([v, filler], axis=0).T

    def build(rb, _):
        rows = pl.ds(pl.multiple_of(rb * 16, 16), 16)
        rows_s = pl.ds(pl.multiple_of(HOP + rb * 16, 16), 16)
        lo, w0, w1 = lo_s[rows, :], w0_s[rows, :], w1_s[rows, :]
        a0 = jnp.zeros((16, 128), I32)
        a1 = jnp.zeros((16, 128), I32)
        for j in range(near_v.shape[0]):
            hit = lo[:, j : j + 1] == lanes
            a0 = a0 + jnp.where(hit, w0[:, j : j + 1], 0)
            a1 = a1 + jnp.where(hit, w1[:, j : j + 1], 0)
        own = jnp.broadcast_to(selfc[rows, :], (16, 128))
        for t in range(SLOTS // 128):
            word = a0 if t < 8 else a1
            v = jnp.right_shift(word, 4 * (t % 8)) & 15
            cols = pl.ds(t * 128, 128)
            amat[rows, cols] = v.astype(F32).astype(BF)
            amat[rows_s, cols] = jnp.where(own == lanes + t * 128, 1.0, 0.0).astype(BF)
        return 0

    lax.fori_loop(0, HOP // 16, build, 0)

    for cp in c_idb:
        cp.wait()
    selfb_t = selfb_v[...].T
    invb_t = (1.0 / cntb_v[...].astype(F32)).T
    for g in range(SEEDS // 128):
        cols = pl.ds(g * 128, 128)
        invb[cols, :] = invb_t[:, g : g + 1]
        nb = nearb_v[:, cols]
        nb = jnp.where(lax.broadcasted_iota(I32, nb.shape, 0) < cntb_v[pl.ds(g, 1), :], nb, -1)
        nb = jnp.concatenate([nb, jnp.full((8 - nb.shape[0], 128), -1, I32)], axis=0).T
        sb = selfb_t[:, g : g + 1]
        for s in range(8):
            for t in range(HOP // 128):
                tot = jnp.zeros((16, 128), F32)
                for j in range(nearb_v.shape[0]):
                    tot = tot + jnp.where(nb[s * 16 : s * 16 + 16, j : j + 1] == lanes + t * 128, 1.0, 0.0)
                bmat[pl.ds(g * 128 + s * 16, 16), pl.ds(t * 128, 128)] = tot.astype(BF)
                hit = sb[s * 16 : s * 16 + 16] == lanes + t * 128
                bmat[pl.ds(SEEDS + g * 128 + s * 16, 16), pl.ds(t * 128, 128)] = jnp.where(
                    hit, 1.0, 0.0
                ).astype(BF)

    def add_up(k, first):
        xk = xbuf[pl.ds(k * NP, NP)].reshape(BLK, FH)

        def rows_of(b, _):
            rows = pl.ds(pl.multiple_of(b * 512, 512), 512)
            cols = pl.ds(pl.multiple_of(k * BLK, BLK), BLK)
            tot = jnp.dot(amat[rows, cols], xk, preferred_element_type=F32)
            if first:
                acc[rows, :] = tot
            else:
                acc[rows, :] += tot
            return 0

        lax.fori_loop(0, SLOTS // 512, rows_of, 0)

    def arrived(k, n):
        pltpu.make_async_remote_copy(
            src_ref=stag.at[pl.ds(0, n)], dst_ref=xbuf.at[pl.ds(k * NP, n)],
            send_sem=fsem.at[0], recv_sem=frsem.at[k], device_id=mate, device_id_type=MESH,
        ).wait_recv()

    for i, p in enumerate(PAIRS):
        arrived(p, NP if p else NP - 1)
        add_up(p, i == 0)

    for cp in c_bias + c_w:
        cp.wait()
    for cp in w_out:
        cp.wait_recv()

    def half_copy(b):
        return pltpu.make_async_remote_copy(
            src_ref=psend.at[b], dst_ref=precv.at[b], send_sem=qsem.at[b], recv_sem=qrsem.at[b],
            device_id=mate, device_id_type=MESH,
        )

    for b in range(NBLK):
        rows = pl.ds(b * BLK, BLK)
        own = acc[pl.ds(HOP + b * BLK, BLK), :].astype(BF)
        mean = (acc[rows, :] * invc[rows, :]).astype(BF)
        both = jnp.concatenate([own, mean], axis=1)
        for h in range(2):
            v = jnp.dot(both, wa_v[h], preferred_element_type=F32)
            part[rows, pl.ds(h * HH, HH)] = v
            psend[b, :, pl.ds(h * HH, HH)] = v.astype(BF)
        half_copy(b).start()

    for b in range(NBLK):
        rows = pl.ds(b * BLK, BLK)
        half_copy(b).wait_recv()
        v = part[rows, :] + precv[b].astype(F32) + ba_v[...]
        hid = jnp.maximum(v, 0.0).astype(BF)
        tot = jnp.dot(bmat[:, pl.ds(b * BLK, BLK)], hid, preferred_element_type=F32)
        if b == 0:
            accb[...] = tot
        else:
            accb[...] += tot

    own = accb[pl.ds(SEEDS, SEEDS), :].astype(BF)
    mean = (accb[pl.ds(0, SEEDS), :] * invb[...]).astype(BF)
    both = jnp.concatenate([own, mean], axis=1)

    def state_of(h):
        v = jnp.dot(both, wb_v[h], preferred_element_type=F32) + bb_v[:, pl.ds(pl.multiple_of(h * HH, HH), HH)]
        return jnp.maximum(v, 0.0)

    s0 = state_of(c)
    s1 = state_of(1 - c)
    squares = jnp.sum(s0 * s0, axis=1, keepdims=True) + jnp.sum(s1 * s1, axis=1, keepdims=True)
    out[...] = (s0 * jnp.sqrt(jnp.float32(H)) / jnp.sqrt(squares + H)).astype(BF)

    got.wait_send()
    for n in SERVE[1:]:
        plane_copy(n).wait_send()
    for cp in w_out:
        cp.wait_send()
    for k in range(NZ):
        n = NP - 1 if k == 0 else NP
        pltpu.make_async_remote_copy(
            src_ref=stag.at[pl.ds(k * NP, n)], dst_ref=xbuf.at[pl.ds(0, n)],
            send_sem=fsem.at[k], recv_sem=frsem.at[0], device_id=mate, device_id_type=MESH,
        ).wait_send()
    for b in range(NBLK):
        half_copy(b).wait_send()


def shards(
    table, weight_a, bias_a, weight_b, bias_b, requests,
    near_a, self_a, count_a, near_b, self_b, count_b,
):
    vmem = pl.BlockSpec(memory_space=pltpu.VMEM)
    hbm = pl.BlockSpec(memory_space=pl.ANY)
    dma = pltpu.SemaphoreType.DMA
    return pl.pallas_call(
        kernel,
        name="sage",
        out_shape=jax.ShapeDtypeStruct((SEEDS, HH), BF),
        in_specs=[hbm] * 12,
        out_specs=vmem,
        scratch_shapes=[
            pltpu.VMEM((NODE, FH), BF),
            pltpu.VMEM((2, 2 * FH, HH), BF),
            pltpu.VMEM((2, 2 * H, HH), BF),
            pltpu.VMEM((1, H), F32),
            pltpu.VMEM((1, H), F32),
            pltpu.VMEM((16, 128), I32),
            pltpu.VMEM((10, HOP), I32),
            pltpu.VMEM((HOP // 128, 128), I32),
            pltpu.VMEM((HOP // 128, 128), I32),
            pltpu.VMEM((5, SEEDS), I32),
            pltpu.VMEM((SEEDS // 128, 128), I32),
            pltpu.VMEM((SEEDS // 128, 128), I32),
            pltpu.VMEM((128, 16), I32),
            pltpu.VMEM((2, NZ, 1, 128), I32),
            pltpu.VMEM((2, NZ, 1, 128), I32),
            pltpu.VMEM((NP, NZ, 1, 128), I32),
            pltpu.VMEM((128, NZ), I32),
            pltpu.VMEM((128, NODE), BF),
            pltpu.VMEM((NZ * NP, ROWS, FH), BF),
            pltpu.VMEM((NZ * NP, ROWS, FH), BF),
            pltpu.VMEM((2 * HOP, SLOTS), BF),
            pltpu.VMEM((2 * HOP, FH), F32),
            pltpu.VMEM((HOP, 16), I32),
            pltpu.VMEM((HOP, 16), I32),
            pltpu.VMEM((HOP, 16), I32),
            pltpu.VMEM((HOP, 1), I32),
            pltpu.VMEM((HOP, 1), F32),
            pltpu.VMEM((HOP, H), F32),
            pltpu.VMEM((NBLK, BLK, H), BF),
            pltpu.VMEM((NBLK, BLK, H), BF),
            pltpu.VMEM((2 * SEEDS, HOP), BF),
            pltpu.VMEM((2 * SEEDS, H), F32),
            pltpu.VMEM((SEEDS, 1), F32),
            dma((13,)),
            dma((3,)),
            dma((3,)),
            dma((NP,)),
            dma((NP,)),
            dma,
            dma,
            dma((NZ,)),
            dma((NZ,)),
            dma((NBLK,)),
            dma((NBLK,)),
        ],
        compiler_params=pltpu.CompilerParams(
            collective_id=0, has_side_effects=True, vmem_limit_bytes=50000 * 1024
        ),
    )(
        *(
            pltpu.with_memory_space_constraint(v, pltpu.HBM)
            for v in (
        table,
        weight_a,
        bias_a.reshape(1, H),
        weight_b,
        bias_b.reshape(1, H),
        jnp.swapaxes(requests[0], 0, 1),
        near_a.T,
        self_a.reshape(HOP // 128, 128),
        count_a.reshape(HOP // 128, 128),
        near_b.T,
        self_b.reshape(SEEDS // 128, 128),
        count_b.reshape(SEEDS // 128, 128),
            )
        )
    )


def solution(mesh):
    placed = (
        P("dom", "mp"),
        P(None, "mp"),
        P(),
        P(None, "mp"),
        P(),
        P("dom", None, None),
        P("dom", None),
        P("dom"),
        P("dom"),
        P("dom", None),
        P("dom"),
        P("dom"),
    )
    return jax.shard_map(
        shards, mesh=mesh, in_specs=placed, out_specs=P("dom", "mp"), check_vma=False
    )
```

```python
import functools

import jax
import jax.numpy as jnp
from jax import lax
from jax.experimental import pallas as pl
from jax.experimental.pallas import tpu as pltpu
from jax.sharding import PartitionSpec as P

F = 768
H = 512
FH = 384
HH = 256
NX, NY, NZ = 4, 4, 8
NP = NX * NY
ROWS = 16
HOP = 1024
SLOTS = 2048
SEEDS = 256
NODE = 4096
OFFSET = (
    (0, 0), (0, 2), (0, 1), (0, 3), (1, 0), (3, 0), (1, 1), (3, 3),
    (1, 3), (3, 1), (2, 0), (2, 2), (1, 2), (3, 2), (2, 1), (2, 3),
)
BACK = tuple(OFFSET.index(((4 - a) % 4, (4 - b) % 4)) for a, b in OFFSET)
SERVE = (0, 2, 3, 11, 12, 13, 14, 15, 6, 7, 8, 9, 10, 1, 4, 5)
PAIRS = (1, 6, 7, 3, 4, 5, 0, 2)
BLK = 256
NBLK = HOP // BLK
MESH = pl.DeviceIdType.MESH
I32 = jnp.int32
F32 = jnp.float32
BF = jnp.bfloat16


def look(values, i):
    return sum(v * (i == n).astype(I32) for n, v in enumerate(values) if v)


def kernel(
    table, wa, ba, wb, bb, req, near_a, self_a, cnt_a, near_b, self_b, cnt_b,
    out,
    table_v, wa_v, wb_v, ba_v, bb_v, req_v, near_v, selfa_v, cnta_v, nearb_v, selfb_v, cntb_v,
    req_t, req2, zreq, preq, tz, pick, stag, xbuf, amat, acc, lo_s, w0_s, w1_s, selfc, invc,
    part, psend, precv, bmat, accb, invb,
    lsem, wsem, wrsem, psem, prsem, zsem, zrsem, fsem, frsem, qsem, qrsem,
):
    d = lax.axis_index("dom")
    c = lax.axis_index("mp")
    x, z, y = d // (NZ * NY), (d // NY) % NZ, d % NY
    qme = x * NY + y
    mate = (d, 1 - c)

    def at_plane(n):
        a, b = OFFSET[n] if isinstance(n, int) else (look([o[0] for o in OFFSET], n), look([o[1] for o in OFFSET], n))
        tx, ty = (x + a) % NX, (y + b) % NY
        return tx, ty, tx * NY + ty

    def dev(tx, tz_, ty):
        return (tx * (NZ * NY) + tz_ * NY + ty, c)

    local = []

    def bring(src, dst):
        cp = pltpu.make_async_copy(src, dst, lsem.at[len(local)])
        cp.start()
        local.append(cp)
        return cp

    c_req = bring(req, req_v)
    c_idx = [bring(near_a, near_v), bring(self_a, selfa_v), bring(cnt_a, cnta_v)]
    c_tab = bring(table, table_v)
    c_idb = [bring(near_b, nearb_v), bring(self_b, selfb_v), bring(cnt_b, cntb_v)]
    c_bias = [bring(ba, ba_v), bring(bb, bb_v)]
    mine = pl.multiple_of(c * FH, 128)
    c_w = [
        bring(wa.at[pl.ds(mine, FH)], wa_v.at[c, pl.ds(0, FH)]),
        bring(wa.at[pl.ds(F + mine, FH)], wa_v.at[c, pl.ds(FH, FH)]),
        bring(wb, wb_v.at[c]),
    ]

    barrier = pltpu.get_barrier_semaphore()
    for m in range(1, NP):
        tx, ty, _ = at_plane(m)
        pl.semaphore_signal(barrier, inc=1, device_id=dev(tx, z, ty), device_id_type=MESH)
    for j in range(1, NZ):
        pl.semaphore_signal(barrier, inc=1, device_id=dev(x, (z + j) % NZ, y), device_id_type=MESH)
    pl.semaphore_signal(barrier, inc=1, device_id=mate, device_id_type=MESH)

    c_req.wait()
    req_t[...] = req_v[...].T
    for h in range(2):
        req2[h] = jnp.concatenate(
            [
                req_t[pl.ds((q // NY) * 32 + q % NY, NZ, stride=NY), :]
                for q in range(h * 8, h * 8 + 8)
            ],
            axis=1,
        ).reshape(NZ, 1, 128)

    pl.semaphore_wait(barrier, NP - 1 + NZ - 1 + 1)

    for j in (4, 3, 5, 2, 6, 1, 7):
        pltpu.make_async_remote_copy(
            src_ref=req2.at[:, (z + j) % NZ], dst_ref=zreq.at[:, NZ - j], send_sem=zsem, recv_sem=zrsem,
            device_id=dev(x, (z + j) % NZ, y), device_id_type=MESH,
        ).start()
    zreq[:, 0] = req2[:, z]

    lanes = lax.broadcasted_iota(I32, (16, 128), 1)

    got = pltpu.make_async_remote_copy(
        src_ref=req2.at[:, pl.ds(0, NZ - 1)], dst_ref=zreq.at[:, pl.ds(0, NZ - 1)],
        send_sem=zsem, recv_sem=zrsem, device_id=mate, device_id_type=MESH,
    )
    got.wait_recv()

    def plane_copy(n):
        tx, ty, q = at_plane(n)
        return pltpu.make_async_remote_copy(
            src_ref=zreq.at[q // 8], dst_ref=preq.at[BACK[n]],
            send_sem=psem.at[n], recv_sem=prsem.at[BACK[n]],
            device_id=dev(tx, z, ty), device_id_type=MESH,
        )

    for n in SERVE[1:]:
        plane_copy(n).start()
    preq[0] = zreq[qme // 8]

    other = pl.multiple_of((1 - c) * FH, 128)
    w_out = []
    for i, (src, dst) in enumerate(
        (
            (wa.at[pl.ds(other, FH)], wa_v.at[c, pl.ds(0, FH)]),
            (wa.at[pl.ds(F + other, FH)], wa_v.at[c, pl.ds(FH, FH)]),
            (wb, wb_v.at[c]),
        )
    ):
        cp = pltpu.make_async_remote_copy(
            src_ref=src, dst_ref=dst, send_sem=wsem.at[i], recv_sem=wrsem.at[i],
            device_id=mate, device_id_type=MESH,
        )
        cp.start()
        w_out.append(cp)

    c_tab.wait()

    def feature_send(n, j):
        tx, ty, _ = at_plane(n)
        back = look(BACK, n)
        return pltpu.make_async_remote_copy(
            src_ref=stag.at[n * NZ + j], dst_ref=xbuf.at[back * NZ + (NZ - j) % NZ],
            send_sem=fsem.at[n // 2], recv_sem=frsem.at[back // 2],
            device_id=dev(tx, (z + j) % NZ, ty), device_id_type=MESH,
        )

    def gather(n):
        tz[...] = preq[n].reshape(NZ, 128).T
        idx = tz[pl.ds(pl.multiple_of((qme % 8) * 16, 16), 16), :]
        for j in range(NZ):
            want = jnp.broadcast_to(idx[:, j : j + 1], (16, 128))
            for t in range(NODE // 128):
                pick[pl.ds(j * 16, 16), pl.ds(t * 128, 128)] = jnp.where(
                    want == lanes + t * 128, 1.0, 0.0
                ).astype(BF)
        rows = jnp.dot(pick[...], table_v[...], preferred_element_type=F32)
        stag[pl.ds(n * NZ, NZ)] = rows.astype(BF).reshape(NZ, ROWS, FH)

    def serve(i, _):
        n = look(SERVE, i)

        @pl.when(n > 0)
        def _():
            pltpu.make_async_remote_copy(
                src_ref=zreq.at[0], dst_ref=preq.at[n], send_sem=psem.at[0], recv_sem=prsem.at[n],
                device_id=mate, device_id_type=MESH,
            ).wait_recv()

        gather(n)
        for j in (4, 3, 5, 2, 6, 1, 7):
            feature_send(n, j).start()

        @pl.when(n > 0)
        def _():
            feature_send(n, 0).start()

        return 0

    lax.fori_loop(0, NP, serve, 0)
    xbuf[0] = stag[0]

    for cp in c_idx:
        cp.wait()

    def place(s):
        kk = (((s >> 6) & 7) - z) & 7
        m = ((((s >> 9) - x) & 3) << 2) | ((((s >> 4) & 3) - y) & 3)
        rank = sum(jnp.where(m == a * NY + b, n, 0) for n, (a, b) in enumerate(OFFSET) if n)
        return (rank << 7) | (kk << 4) | (s & 15)

    self_t = place(selfa_v[...]).T
    inv_t = (1.0 / cnta_v[...].astype(F32)).T
    filler = jnp.zeros((16 - near_v.shape[0], 128), I32)
    for g in range(HOP // 128):
        rows = pl.ds(g * 128, 128)
        selfc[rows, :] = self_t[:, g : g + 1]
        invc[rows, :] = inv_t[:, g : g + 1]
        p = place(near_v[:, rows])
        valid = lax.broadcasted_iota(I32, p.shape, 0) < cnta_v[pl.ds(g, 1), :]
        one = jnp.left_shift(jnp.ones_like(p), ((p >> 7) & 7) * 4)
        w0 = jnp.where(valid & (p < 1024), one, 0)
        w1 = jnp.where(valid & (p >= 1024), one, 0)
        for to, v in ((lo_s, p & 127), (w0_s, w0), (w1_s, w1)):
            to[rows, :] = jnp.concatenate([v, filler], axis=0).T

    def build(rb, _):
        rows = pl.ds(pl.multiple_of(rb * 16, 16), 16)
        rows_s = pl.ds(pl.multiple_of(HOP + rb * 16, 16), 16)
        lo, w0, w1 = lo_s[rows, :], w0_s[rows, :], w1_s[rows, :]
        a0 = jnp.zeros((16, 128), I32)
        a1 = jnp.zeros((16, 128), I32)
        for j in range(near_v.shape[0]):
            hit = lo[:, j : j + 1] == lanes
            a0 = a0 + jnp.where(hit, w0[:, j : j + 1], 0)
            a1 = a1 + jnp.where(hit, w1[:, j : j + 1], 0)
        own = jnp.broadcast_to(selfc[rows, :], (16, 128))
        for t in range(SLOTS // 128):
            word = a0 if t < 8 else a1
            v = jnp.right_shift(word, 4 * (t % 8)) & 15
            cols = pl.ds(t * 128, 128)
            amat[rows, cols] = v.astype(F32).astype(BF)
            amat[rows_s, cols] = jnp.where(own == lanes + t * 128, 1.0, 0.0).astype(BF)
        return 0

    lax.fori_loop(0, HOP // 16, build, 0)

    for cp in c_idb:
        cp.wait()
    selfb_t = selfb_v[...].T
    invb_t = (1.0 / cntb_v[...].astype(F32)).T
    for g in range(SEEDS // 128):
        cols = pl.ds(g * 128, 128)
        invb[cols, :] = invb_t[:, g : g + 1]
        nb = nearb_v[:, cols]
        nb = jnp.where(lax.broadcasted_iota(I32, nb.shape, 0) < cntb_v[pl.ds(g, 1), :], nb, -1)
        nb = jnp.concatenate([nb, jnp.full((8 - nb.shape[0], 128), -1, I32)], axis=0).T
        sb = selfb_t[:, g : g + 1]
        for s in range(8):
            for t in range(HOP // 128):
                tot = jnp.zeros((16, 128), F32)
                for j in range(nearb_v.shape[0]):
                    tot = tot + jnp.where(nb[s * 16 : s * 16 + 16, j : j + 1] == lanes + t * 128, 1.0, 0.0)
                bmat[pl.ds(g * 128 + s * 16, 16), pl.ds(t * 128, 128)] = tot.astype(BF)
                hit = sb[s * 16 : s * 16 + 16] == lanes + t * 128
                bmat[pl.ds(SEEDS + g * 128 + s * 16, 16), pl.ds(t * 128, 128)] = jnp.where(
                    hit, 1.0, 0.0
                ).astype(BF)

    def add_up(k, first):
        xk = xbuf[pl.ds(k * NP, NP)].reshape(BLK, FH)

        def rows_of(b, _):
            rows = pl.ds(pl.multiple_of(b * 512, 512), 512)
            cols = pl.ds(pl.multiple_of(k * BLK, BLK), BLK)
            tot = jnp.dot(amat[rows, cols], xk, preferred_element_type=F32)
            if first:
                acc[rows, :] = tot
            else:
                acc[rows, :] += tot
            return 0

        lax.fori_loop(0, SLOTS // 512, rows_of, 0)

    def arrived(k, n):
        pltpu.make_async_remote_copy(
            src_ref=stag.at[pl.ds(0, n)], dst_ref=xbuf.at[pl.ds(k * NP, n)],
            send_sem=fsem.at[0], recv_sem=frsem.at[k], device_id=mate, device_id_type=MESH,
        ).wait_recv()

    for i, p in enumerate(PAIRS):
        arrived(p, NP if p else NP - 1)
        if i < NZ - 1:
            add_up(p, i == 0)
    last = PAIRS[-1]
    x_last = xbuf[pl.ds(last * NP, NP)].reshape(BLK, FH)

    def finished(lo):
        at = pl.ds(lo, BLK)
        return acc[at, :] + jnp.dot(amat[at, pl.ds(last * BLK, BLK)], x_last, preferred_element_type=F32)

    for cp in c_bias + c_w:
        cp.wait()
    for cp in w_out:
        cp.wait_recv()

    def half_copy(b):
        return pltpu.make_async_remote_copy(
            src_ref=psend.at[b], dst_ref=precv.at[b], send_sem=qsem.at[b], recv_sem=qrsem.at[b],
            device_id=mate, device_id_type=MESH,
        )

    for b in range(NBLK):
        rows = pl.ds(b * BLK, BLK)
        own = finished(HOP + b * BLK).astype(BF)
        mean = (finished(b * BLK) * invc[rows, :]).astype(BF)
        both = jnp.concatenate([own, mean], axis=1)
        for h in range(2):
            v = jnp.dot(both, wa_v[h], preferred_element_type=F32)
            part[rows, pl.ds(h * HH, HH)] = v
            psend[b, :, pl.ds(h * HH, HH)] = v.astype(BF)
        half_copy(b).start()

    for b in range(NBLK):
        rows = pl.ds(b * BLK, BLK)
        half_copy(b).wait_recv()
        v = part[rows, :] + precv[b].astype(F32) + ba_v[...]
        hid = jnp.maximum(v, 0.0).astype(BF)
        tot = jnp.dot(bmat[:, pl.ds(b * BLK, BLK)], hid, preferred_element_type=F32)
        if b == 0:
            accb[...] = tot
        else:
            accb[...] += tot

    own = accb[pl.ds(SEEDS, SEEDS), :].astype(BF)
    mean = (accb[pl.ds(0, SEEDS), :] * invb[...]).astype(BF)
    both = jnp.concatenate([own, mean], axis=1)

    def state_of(h):
        v = jnp.dot(both, wb_v[h], preferred_element_type=F32) + bb_v[:, pl.ds(pl.multiple_of(h * HH, HH), HH)]
        return jnp.maximum(v, 0.0)

    s0 = state_of(c)
    s1 = state_of(1 - c)
    squares = jnp.sum(s0 * s0, axis=1, keepdims=True) + jnp.sum(s1 * s1, axis=1, keepdims=True)
    out[...] = (s0 * jnp.sqrt(jnp.float32(H)) / jnp.sqrt(squares + H)).astype(BF)

    got.wait_send()
    for n in SERVE[1:]:
        plane_copy(n).wait_send()
    for cp in w_out:
        cp.wait_send()
    for k in range(NZ):
        n = NP - 1 if k == 0 else NP
        pltpu.make_async_remote_copy(
            src_ref=stag.at[pl.ds(k * NP, n)], dst_ref=xbuf.at[pl.ds(0, n)],
            send_sem=fsem.at[k], recv_sem=frsem.at[0], device_id=mate, device_id_type=MESH,
        ).wait_send()
    for b in range(NBLK):
        half_copy(b).wait_send()


def shards(
    table, weight_a, bias_a, weight_b, bias_b, requests,
    near_a, self_a, count_a, near_b, self_b, count_b,
):
    vmem = pl.BlockSpec(memory_space=pltpu.VMEM)
    hbm = pl.BlockSpec(memory_space=pl.ANY)
    dma = pltpu.SemaphoreType.DMA
    return pl.pallas_call(
        kernel,
        name="sage",
        out_shape=jax.ShapeDtypeStruct((SEEDS, HH), BF),
        in_specs=[hbm] * 12,
        out_specs=vmem,
        scratch_shapes=[
            pltpu.VMEM((NODE, FH), BF),
            pltpu.VMEM((2, 2 * FH, HH), BF),
            pltpu.VMEM((2, 2 * H, HH), BF),
            pltpu.VMEM((1, H), F32),
            pltpu.VMEM((1, H), F32),
            pltpu.VMEM((16, 128), I32),
            pltpu.VMEM((10, HOP), I32),
            pltpu.VMEM((HOP // 128, 128), I32),
            pltpu.VMEM((HOP // 128, 128), I32),
            pltpu.VMEM((5, SEEDS), I32),
            pltpu.VMEM((SEEDS // 128, 128), I32),
            pltpu.VMEM((SEEDS // 128, 128), I32),
            pltpu.VMEM((128, 16), I32),
            pltpu.VMEM((2, NZ, 1, 128), I32),
            pltpu.VMEM((2, NZ, 1, 128), I32),
            pltpu.VMEM((NP, NZ, 1, 128), I32),
            pltpu.VMEM((128, NZ), I32),
            pltpu.VMEM((128, NODE), BF),
            pltpu.VMEM((NZ * NP, ROWS, FH), BF),
            pltpu.VMEM((NZ * NP, ROWS, FH), BF),
            pltpu.VMEM((2 * HOP, SLOTS), BF),
            pltpu.VMEM((2 * HOP, FH), F32),
            pltpu.VMEM((HOP, 16), I32),
            pltpu.VMEM((HOP, 16), I32),
            pltpu.VMEM((HOP, 16), I32),
            pltpu.VMEM((HOP, 1), I32),
            pltpu.VMEM((HOP, 1), F32),
            pltpu.VMEM((HOP, H), F32),
            pltpu.VMEM((NBLK, BLK, H), BF),
            pltpu.VMEM((NBLK, BLK, H), BF),
            pltpu.VMEM((2 * SEEDS, HOP), BF),
            pltpu.VMEM((2 * SEEDS, H), F32),
            pltpu.VMEM((SEEDS, 1), F32),
            dma((13,)),
            dma((3,)),
            dma((3,)),
            dma((NP,)),
            dma((NP,)),
            dma,
            dma,
            dma((NZ,)),
            dma((NZ,)),
            dma((NBLK,)),
            dma((NBLK,)),
        ],
        compiler_params=pltpu.CompilerParams(
            collective_id=0, has_side_effects=True, vmem_limit_bytes=50000 * 1024
        ),
    )(
        *(
            pltpu.with_memory_space_constraint(v, pltpu.HBM)
            for v in (
        table,
        weight_a,
        bias_a.reshape(1, H),
        weight_b,
        bias_b.reshape(1, H),
        jnp.swapaxes(requests[0], 0, 1),
        near_a.T,
        self_a.reshape(HOP // 128, 128),
        count_a.reshape(HOP // 128, 128),
        near_b.T,
        self_b.reshape(SEEDS // 128, 128),
        count_b.reshape(SEEDS // 128, 128),
            )
        )
    )


def solution(mesh):
    placed = (
        P("dom", "mp"),
        P(None, "mp"),
        P(),
        P(None, "mp"),
        P(),
        P("dom", None, None),
        P("dom", None),
        P("dom"),
        P("dom"),
        P("dom", None),
        P("dom"),
        P("dom"),
    )
    return jax.shard_map(
        shards, mesh=mesh, in_specs=placed, out_specs=P("dom", "mp"), check_vma=False
    )
```

```python
import functools

import jax
import jax.numpy as jnp
from jax import lax
from jax.experimental import pallas as pl
from jax.experimental.pallas import tpu as pltpu
from jax.sharding import PartitionSpec as P

F = 768
H = 512
FH = 384
HH = 256
NX, NY, NZ = 4, 4, 8
NP = NX * NY
ROWS = 16
HOP = 1024
SLOTS = 2048
SEEDS = 256
NODE = 4096
OFFSET = (
    (0, 0), (0, 2), (0, 1), (0, 3), (1, 0), (3, 0), (1, 1), (3, 3),
    (1, 3), (3, 1), (2, 0), (2, 2), (1, 2), (3, 2), (2, 1), (2, 3),
)
BACK = tuple(OFFSET.index(((4 - a) % 4, (4 - b) % 4)) for a, b in OFFSET)
SERVE = (0, 2, 3, 11, 12, 13, 14, 15, 6, 7, 8, 9, 10, 1, 4, 5)
PAIRS = (1, 6, 7, 3, 4, 5, 0, 2)
BLK = 256
TAIL = ((0, 384), (384, 384), (768, 128), (896, 128))
NBLK = len(TAIL)
MESH = pl.DeviceIdType.MESH
I32 = jnp.int32
F32 = jnp.float32
BF = jnp.bfloat16


def look(values, i):
    return sum(v * (i == n).astype(I32) for n, v in enumerate(values) if v)


def kernel(
    table, wa, ba, wb, bb, req, near_a, self_a, cnt_a, near_b, self_b, cnt_b,
    out,
    table_v, wa_v, wb_v, ba_v, bb_v, req_v, near_v, selfa_v, cnta_v, nearb_v, selfb_v, cntb_v,
    req_t, req2, zreq, preq, tz, pick, stag, xbuf, amat, acc, lo_s, w0_s, w1_s, selfc, invc,
    part, psend, precv, bmat, accb, invb,
    lsem, wsem, wrsem, psem, prsem, zsem, zrsem, fsem, frsem, qsem, qrsem,
):
    d = lax.axis_index("dom")
    c = lax.axis_index("mp")
    x, z, y = d // (NZ * NY), (d // NY) % NZ, d % NY
    qme = x * NY + y
    mate = (d, 1 - c)

    def at_plane(n):
        a, b = OFFSET[n] if isinstance(n, int) else (look([o[0] for o in OFFSET], n), look([o[1] for o in OFFSET], n))
        tx, ty = (x + a) % NX, (y + b) % NY
        return tx, ty, tx * NY + ty

    def dev(tx, tz_, ty):
        return (tx * (NZ * NY) + tz_ * NY + ty, c)

    local = []

    def bring(src, dst):
        cp = pltpu.make_async_copy(src, dst, lsem.at[len(local)])
        cp.start()
        local.append(cp)
        return cp

    c_req = bring(req, req_v)
    c_idx = [bring(near_a, near_v), bring(self_a, selfa_v), bring(cnt_a, cnta_v)]
    c_tab = bring(table, table_v)
    c_idb = [bring(near_b, nearb_v), bring(self_b, selfb_v), bring(cnt_b, cntb_v)]
    c_bias = [bring(ba, ba_v), bring(bb, bb_v)]
    mine = pl.multiple_of(c * FH, 128)
    c_w = [
        bring(wa.at[pl.ds(mine, FH)], wa_v.at[c, pl.ds(0, FH)]),
        bring(wa.at[pl.ds(F + mine, FH)], wa_v.at[c, pl.ds(FH, FH)]),
        bring(wb, wb_v.at[c]),
    ]

    barrier = pltpu.get_barrier_semaphore()
    for m in range(1, NP):
        tx, ty, _ = at_plane(m)
        pl.semaphore_signal(barrier, inc=1, device_id=dev(tx, z, ty), device_id_type=MESH)
    for j in range(1, NZ):
        pl.semaphore_signal(barrier, inc=1, device_id=dev(x, (z + j) % NZ, y), device_id_type=MESH)
    pl.semaphore_signal(barrier, inc=1, device_id=mate, device_id_type=MESH)

    c_req.wait()
    req_t[...] = req_v[...].T
    for h in range(2):
        req2[h] = jnp.concatenate(
            [
                req_t[pl.ds((q // NY) * 32 + q % NY, NZ, stride=NY), :]
                for q in range(h * 8, h * 8 + 8)
            ],
            axis=1,
        ).reshape(NZ, 1, 128)

    pl.semaphore_wait(barrier, NP - 1 + NZ - 1 + 1)

    for j in (4, 3, 5, 2, 6, 1, 7):
        pltpu.make_async_remote_copy(
            src_ref=req2.at[:, (z + j) % NZ], dst_ref=zreq.at[:, NZ - j], send_sem=zsem, recv_sem=zrsem,
            device_id=dev(x, (z + j) % NZ, y), device_id_type=MESH,
        ).start()
    zreq[:, 0] = req2[:, z]

    lanes = lax.broadcasted_iota(I32, (16, 128), 1)

    got = pltpu.make_async_remote_copy(
        src_ref=req2.at[:, pl.ds(0, NZ - 1)], dst_ref=zreq.at[:, pl.ds(0, NZ - 1)],
        send_sem=zsem, recv_sem=zrsem, device_id=mate, device_id_type=MESH,
    )
    got.wait_recv()

    def plane_copy(n):
        tx, ty, q = at_plane(n)
        return pltpu.make_async_remote_copy(
            src_ref=zreq.at[q // 8], dst_ref=preq.at[BACK[n]],
            send_sem=psem.at[n], recv_sem=prsem.at[BACK[n]],
            device_id=dev(tx, z, ty), device_id_type=MESH,
        )

    for n in SERVE[1:]:
        plane_copy(n).start()
    preq[0] = zreq[qme // 8]

    other = pl.multiple_of((1 - c) * FH, 128)
    w_out = []
    for i, (src, dst) in enumerate(
        (
            (wa.at[pl.ds(other, FH)], wa_v.at[c, pl.ds(0, FH)]),
            (wa.at[pl.ds(F + other, FH)], wa_v.at[c, pl.ds(FH, FH)]),
            (wb, wb_v.at[c]),
        )
    ):
        cp = pltpu.make_async_remote_copy(
            src_ref=src, dst_ref=dst, send_sem=wsem.at[i], recv_sem=wrsem.at[i],
            device_id=mate, device_id_type=MESH,
        )
        cp.start()
        w_out.append(cp)

    c_tab.wait()

    def feature_send(n, j):
        tx, ty, _ = at_plane(n)
        back = look(BACK, n)
        return pltpu.make_async_remote_copy(
            src_ref=stag.at[n * NZ + j], dst_ref=xbuf.at[back * NZ + (NZ - j) % NZ],
            send_sem=fsem.at[n // 2], recv_sem=frsem.at[back // 2],
            device_id=dev(tx, (z + j) % NZ, ty), device_id_type=MESH,
        )

    def gather(n):
        tz[...] = preq[n].reshape(NZ, 128).T
        idx = tz[pl.ds(pl.multiple_of((qme % 8) * 16, 16), 16), :]
        for j in range(NZ):
            want = jnp.broadcast_to(idx[:, j : j + 1], (16, 128))
            for t in range(NODE // 128):
                pick[pl.ds(j * 16, 16), pl.ds(t * 128, 128)] = jnp.where(
                    want == lanes + t * 128, 1.0, 0.0
                ).astype(BF)
        rows = jnp.dot(pick[...], table_v[...], preferred_element_type=F32)
        stag[pl.ds(n * NZ, NZ)] = rows.astype(BF).reshape(NZ, ROWS, FH)

    def serve(i, _):
        n = look(SERVE, i)

        @pl.when(n > 0)
        def _():
            pltpu.make_async_remote_copy(
                src_ref=zreq.at[0], dst_ref=preq.at[n], send_sem=psem.at[0], recv_sem=prsem.at[n],
                device_id=mate, device_id_type=MESH,
            ).wait_recv()

        gather(n)
        for j in (4, 3, 5, 2, 6, 1, 7):
            feature_send(n, j).start()

        @pl.when(n > 0)
        def _():
            feature_send(n, 0).start()

        return 0

    lax.fori_loop(0, NP, serve, 0)
    xbuf[0] = stag[0]

    for cp in c_idx:
        cp.wait()

    def place(s):
        kk = (((s >> 6) & 7) - z) & 7
        m = ((((s >> 9) - x) & 3) << 2) | ((((s >> 4) & 3) - y) & 3)
        rank = sum(jnp.where(m == a * NY + b, n, 0) for n, (a, b) in enumerate(OFFSET) if n)
        return (rank << 7) | (kk << 4) | (s & 15)

    self_t = place(selfa_v[...]).T
    inv_t = (1.0 / cnta_v[...].astype(F32)).T
    filler = jnp.zeros((16 - near_v.shape[0], 128), I32)
    for g in range(HOP // 128):
        rows = pl.ds(g * 128, 128)
        selfc[rows, :] = self_t[:, g : g + 1]
        invc[rows, :] = inv_t[:, g : g + 1]
        p = place(near_v[:, rows])
        valid = lax.broadcasted_iota(I32, p.shape, 0) < cnta_v[pl.ds(g, 1), :]
        one = jnp.left_shift(jnp.ones_like(p), ((p >> 7) & 7) * 4)
        w0 = jnp.where(valid & (p < 1024), one, 0)
        w1 = jnp.where(valid & (p >= 1024), one, 0)
        for to, v in ((lo_s, p & 127), (w0_s, w0), (w1_s, w1)):
            to[rows, :] = jnp.concatenate([v, filler], axis=0).T

    def build(rb, _):
        rows = pl.ds(pl.multiple_of(rb * 16, 16), 16)
        rows_s = pl.ds(pl.multiple_of(HOP + rb * 16, 16), 16)
        lo, w0, w1 = lo_s[rows, :], w0_s[rows, :], w1_s[rows, :]
        a0 = jnp.zeros((16, 128), I32)
        a1 = jnp.zeros((16, 128), I32)
        for j in range(near_v.shape[0]):
            hit = lo[:, j : j + 1] == lanes
            a0 = a0 + jnp.where(hit, w0[:, j : j + 1], 0)
            a1 = a1 + jnp.where(hit, w1[:, j : j + 1], 0)
        own = jnp.broadcast_to(selfc[rows, :], (16, 128))
        for t in range(SLOTS // 128):
            word = a0 if t < 8 else a1
            v = jnp.right_shift(word, 4 * (t % 8)) & 15
            cols = pl.ds(t * 128, 128)
            amat[rows, cols] = v.astype(F32).astype(BF)
            amat[rows_s, cols] = jnp.where(own == lanes + t * 128, 1.0, 0.0).astype(BF)
        return 0

    lax.fori_loop(0, HOP // 16, build, 0)

    for cp in c_idb:
        cp.wait()
    selfb_t = selfb_v[...].T
    invb_t = (1.0 / cntb_v[...].astype(F32)).T
    for g in range(SEEDS // 128):
        cols = pl.ds(g * 128, 128)
        invb[cols, :] = invb_t[:, g : g + 1]
        nb = nearb_v[:, cols]
        nb = jnp.where(lax.broadcasted_iota(I32, nb.shape, 0) < cntb_v[pl.ds(g, 1), :], nb, -1)
        nb = jnp.concatenate([nb, jnp.full((8 - nb.shape[0], 128), -1, I32)], axis=0).T
        sb = selfb_t[:, g : g + 1]
        for s in range(8):
            for t in range(HOP // 128):
                tot = jnp.zeros((16, 128), F32)
                for j in range(nearb_v.shape[0]):
                    tot = tot + jnp.where(nb[s * 16 : s * 16 + 16, j : j + 1] == lanes + t * 128, 1.0, 0.0)
                bmat[pl.ds(g * 128 + s * 16, 16), pl.ds(t * 128, 128)] = tot.astype(BF)
                hit = sb[s * 16 : s * 16 + 16] == lanes + t * 128
                bmat[pl.ds(SEEDS + g * 128 + s * 16, 16), pl.ds(t * 128, 128)] = jnp.where(
                    hit, 1.0, 0.0
                ).astype(BF)

    def add_up(k, first):
        xk = xbuf[pl.ds(k * NP, NP)].reshape(BLK, FH)

        def rows_of(b, _):
            rows = pl.ds(pl.multiple_of(b * 512, 512), 512)
            cols = pl.ds(pl.multiple_of(k * BLK, BLK), BLK)
            tot = jnp.dot(amat[rows, cols], xk, preferred_element_type=F32)
            if first:
                acc[rows, :] = tot
            else:
                acc[rows, :] += tot
            return 0

        lax.fori_loop(0, SLOTS // 512, rows_of, 0)

    def arrived(k, n):
        pltpu.make_async_remote_copy(
            src_ref=stag.at[pl.ds(0, n)], dst_ref=xbuf.at[pl.ds(k * NP, n)],
            send_sem=fsem.at[0], recv_sem=frsem.at[k], device_id=mate, device_id_type=MESH,
        ).wait_recv()

    for i, p in enumerate(PAIRS):
        arrived(p, NP if p else NP - 1)
        if i < NZ - 1:
            add_up(p, i == 0)
    last = PAIRS[-1]
    x_last = xbuf[pl.ds(last * NP, NP)].reshape(BLK, FH)

    def finished(lo, size):
        at = pl.ds(lo, size)
        return acc[at, :] + jnp.dot(amat[at, pl.ds(last * BLK, BLK)], x_last, preferred_element_type=F32)

    for cp in c_bias + c_w:
        cp.wait()
    for cp in w_out:
        cp.wait_recv()

    def half_copy(b):
        return pltpu.make_async_remote_copy(
            src_ref=psend.at[pl.ds(*TAIL[b])], dst_ref=precv.at[pl.ds(*TAIL[b])], send_sem=qsem.at[b], recv_sem=qrsem.at[b],
            device_id=mate, device_id_type=MESH,
        )

    for b, (lo, size) in enumerate(TAIL):
        rows = pl.ds(lo, size)
        own = finished(HOP + lo, size).astype(BF)
        mean = (finished(lo, size) * invc[rows, :]).astype(BF)
        both = jnp.concatenate([own, mean], axis=1)
        for h in range(2):
            v = jnp.dot(both, wa_v[h], preferred_element_type=F32)
            part[rows, pl.ds(h * HH, HH)] = v
            psend[rows, pl.ds(h * HH, HH)] = v.astype(BF)
        half_copy(b).start()

    for b, (lo, size) in enumerate(TAIL):
        rows = pl.ds(lo, size)
        half_copy(b).wait_recv()
        v = part[rows, :] + precv[rows, :].astype(F32) + ba_v[...]
        hid = jnp.maximum(v, 0.0).astype(BF)
        tot = jnp.dot(bmat[:, rows], hid, preferred_element_type=F32)
        if b == 0:
            accb[...] = tot
        else:
            accb[...] += tot

    own = accb[pl.ds(SEEDS, SEEDS), :].astype(BF)
    mean = (accb[pl.ds(0, SEEDS), :] * invb[...]).astype(BF)
    both = jnp.concatenate([own, mean], axis=1)

    def state_of(h):
        v = jnp.dot(both, wb_v[h], preferred_element_type=F32) + bb_v[:, pl.ds(pl.multiple_of(h * HH, HH), HH)]
        return jnp.maximum(v, 0.0)

    s0 = state_of(c)
    s1 = state_of(1 - c)
    squares = jnp.sum(s0 * s0, axis=1, keepdims=True) + jnp.sum(s1 * s1, axis=1, keepdims=True)
    out[...] = (s0 * jnp.sqrt(jnp.float32(H)) / jnp.sqrt(squares + H)).astype(BF)

    got.wait_send()
    for n in SERVE[1:]:
        plane_copy(n).wait_send()
    for cp in w_out:
        cp.wait_send()
    for k in range(NZ):
        n = NP - 1 if k == 0 else NP
        pltpu.make_async_remote_copy(
            src_ref=stag.at[pl.ds(k * NP, n)], dst_ref=xbuf.at[pl.ds(0, n)],
            send_sem=fsem.at[k], recv_sem=frsem.at[0], device_id=mate, device_id_type=MESH,
        ).wait_send()
    for b in range(NBLK):
        half_copy(b).wait_send()


def shards(
    table, weight_a, bias_a, weight_b, bias_b, requests,
    near_a, self_a, count_a, near_b, self_b, count_b,
):
    vmem = pl.BlockSpec(memory_space=pltpu.VMEM)
    hbm = pl.BlockSpec(memory_space=pl.ANY)
    dma = pltpu.SemaphoreType.DMA
    return pl.pallas_call(
        kernel,
        name="sage",
        out_shape=jax.ShapeDtypeStruct((SEEDS, HH), BF),
        in_specs=[hbm] * 12,
        out_specs=vmem,
        scratch_shapes=[
            pltpu.VMEM((NODE, FH), BF),
            pltpu.VMEM((2, 2 * FH, HH), BF),
            pltpu.VMEM((2, 2 * H, HH), BF),
            pltpu.VMEM((1, H), F32),
            pltpu.VMEM((1, H), F32),
            pltpu.VMEM((16, 128), I32),
            pltpu.VMEM((10, HOP), I32),
            pltpu.VMEM((HOP // 128, 128), I32),
            pltpu.VMEM((HOP // 128, 128), I32),
            pltpu.VMEM((5, SEEDS), I32),
            pltpu.VMEM((SEEDS // 128, 128), I32),
            pltpu.VMEM((SEEDS // 128, 128), I32),
            pltpu.VMEM((128, 16), I32),
            pltpu.VMEM((2, NZ, 1, 128), I32),
            pltpu.VMEM((2, NZ, 1, 128), I32),
            pltpu.VMEM((NP, NZ, 1, 128), I32),
            pltpu.VMEM((128, NZ), I32),
            pltpu.VMEM((128, NODE), BF),
            pltpu.VMEM((NZ * NP, ROWS, FH), BF),
            pltpu.VMEM((NZ * NP, ROWS, FH), BF),
            pltpu.VMEM((2 * HOP, SLOTS), BF),
            pltpu.VMEM((2 * HOP, FH), F32),
            pltpu.VMEM((HOP, 16), I32),
            pltpu.VMEM((HOP, 16), I32),
            pltpu.VMEM((HOP, 16), I32),
            pltpu.VMEM((HOP, 1), I32),
            pltpu.VMEM((HOP, 1), F32),
            pltpu.VMEM((HOP, H), F32),
            pltpu.VMEM((HOP, H), BF),
            pltpu.VMEM((HOP, H), BF),
            pltpu.VMEM((2 * SEEDS, HOP), BF),
            pltpu.VMEM((2 * SEEDS, H), F32),
            pltpu.VMEM((SEEDS, 1), F32),
            dma((13,)),
            dma((3,)),
            dma((3,)),
            dma((NP,)),
            dma((NP,)),
            dma,
            dma,
            dma((NZ,)),
            dma((NZ,)),
            dma((NBLK,)),
            dma((NBLK,)),
        ],
        compiler_params=pltpu.CompilerParams(
            collective_id=0, has_side_effects=True, vmem_limit_bytes=50000 * 1024
        ),
    )(
        *(
            pltpu.with_memory_space_constraint(v, pltpu.HBM)
            for v in (
        table,
        weight_a,
        bias_a.reshape(1, H),
        weight_b,
        bias_b.reshape(1, H),
        jnp.swapaxes(requests[0], 0, 1),
        near_a.T,
        self_a.reshape(HOP // 128, 128),
        count_a.reshape(HOP // 128, 128),
        near_b.T,
        self_b.reshape(SEEDS // 128, 128),
        count_b.reshape(SEEDS // 128, 128),
            )
        )
    )


def solution(mesh):
    placed = (
        P("dom", "mp"),
        P(None, "mp"),
        P(),
        P(None, "mp"),
        P(),
        P("dom", None, None),
        P("dom", None),
        P("dom"),
        P("dom"),
        P("dom", None),
        P("dom"),
        P("dom"),
    )
    return jax.shard_map(
        shards, mesh=mesh, in_specs=placed, out_specs=P("dom", "mp"), check_vma=False
    )
```
